32 devices in a mesh: data: 1 (over z), seq: 4 (over y), dap: 8 (over x, core).
Axes of the slice: x: 4, y: 4, z: 1, core: 2. Of those that a mesh axis runs over, the one named last changes fastest.
The devices are a block of a 4x4x8 slice.
Arguments:
- msa_act: bfloat16 [2048, 256, 64], P(('data', 'seq'), 'dap')
- msa_mask: int32 [2048, 256], P('data')
- pair_act: float32 [256, 256, 128], P(('data', 'dap'))
- ln_gamma: bfloat16 [64], replicated
- ln_beta: bfloat16 [64], replicated
- w_left: bfloat16 [64, 32], replicated
- b_left: bfloat16 [32], replicated
- w_right: bfloat16 [64, 32], replicated
- b_right: bfloat16 [32], replicated
- w_out: bfloat16 [1024, 128], replicated
- b_out: bfloat16 [128], replicated
Outputs:
- output 1: float32 [256, 256, 128], P(('data', 'dap'))
- output 2: bfloat16 [2048, 256, 64], P(('data', 'seq', 'dap'))
All inputs are finite; a program needn't handle non-finite values.
Results may differ from the reference program's by a relative error of at most 0.0120149.
Values are sent between devices in bfloat16 or wider.
A program may use at most 768 MiB of HBM per device.

```python
import math
import jax
import jax.numpy as jnp
from jax import lax

S = 2048
N = 256
CM = 64
CH = 32
CZ = 128
ROW_BLOCK = math.gcd(N, 16)


def setup_inputs(seed: int = 0, part: int = 0) -> dict:
    root_key = jax.random.key(seed)
    shared_root, part_root = jax.random.split(root_key)
    part_key = jax.random.fold_in(part_root, part)
    part_keys = jax.random.split(part_key, 5)
    weight_keys = jax.random.split(shared_root, 8)
    bias_scale = 0.5 * S ** -0.25
    msa_act = jax.random.normal(part_keys[0], (S, N, CM), jnp.float32).astype(jnp.bfloat16)
    col_level = jax.random.randint(part_keys[1], (N,), 8, 16)
    row_shift = jax.random.randint(part_keys[2], (S,), -2, 3)
    draw_mask = jax.random.randint(part_keys[3], (S, N), 0, 16)
    kept_mask = (draw_mask < col_level[None, :] + row_shift[:, None]).astype(jnp.int32)
    first_row = (jnp.arange(S) == 0).astype(jnp.int32)[:, None]
    msa_mask = jnp.maximum(kept_mask, first_row)
    pair_act = 0.5 * jax.random.normal(part_keys[4], (N, N, CZ), jnp.float32)
    ln_gamma = (1.0 + 0.3 * jax.random.normal(weight_keys[0], (CM,), jnp.float32)).astype(jnp.bfloat16)
    ln_beta = (bias_scale * jax.random.normal(weight_keys[1], (CM,), jnp.float32)).astype(jnp.bfloat16)
    w_left = (jax.random.normal(weight_keys[2], (CM, CH), jnp.float32) * CM ** -0.5).astype(jnp.bfloat16)
    b_left = (bias_scale * jax.random.normal(weight_keys[3], (CH,), jnp.float32)).astype(jnp.bfloat16)
    w_right = (jax.random.normal(weight_keys[4], (CM, CH), jnp.float32) * CM ** -0.5).astype(jnp.bfloat16)
    b_right = (bias_scale * jax.random.normal(weight_keys[5], (CH,), jnp.float32)).astype(jnp.bfloat16)
    w_out = (jax.random.normal(weight_keys[6], (CH * CH, CZ), jnp.float32) * (0.5 * math.sqrt(S) / CH)).astype(jnp.bfloat16)
    b_out = (0.25 * S * jax.random.normal(weight_keys[7], (CZ,), jnp.float32)).astype(jnp.bfloat16)
    return {'msa_act': msa_act, 'msa_mask': msa_mask, 'pair_act': pair_act, 'ln_gamma': ln_gamma, 'ln_beta': ln_beta, 'w_left': w_left, 'b_left': b_left, 'w_right': w_right, 'b_right': b_right, 'w_out': w_out, 'b_out': b_out}


def layer_norm(msa_act, ln_gamma, ln_beta):
    act_f32 = msa_act.astype(jnp.float32)
    mean_val = jnp.mean(act_f32, axis=-1, keepdims=True)
    centered = act_f32 - mean_val
    var_val = jnp.mean(centered * centered, axis=-1, keepdims=True)
    normed = centered * lax.rsqrt(var_val + 1e-5)
    return (normed * ln_gamma.astype(jnp.float32) + ln_beta.astype(jnp.float32)).astype(jnp.bfloat16)


def project(normed, weight, bias_vec, mask_f32):
    flat_act = normed.reshape(-1, normed.shape[-1])
    out_f32 = jnp.dot(flat_act, weight, preferred_element_type=jnp.float32) + bias_vec.astype(jnp.float32)
    return (out_f32.reshape(normed.shape[:-1] + (weight.shape[1],)) * mask_f32[:, :, None]).astype(jnp.bfloat16)


def reference(msa_act, msa_mask, pair_act, ln_gamma, ln_beta, w_left, b_left, w_right, b_right, w_out, b_out):
    normed = layer_norm(msa_act, ln_gamma, ln_beta)
    mask_f32 = msa_mask.astype(jnp.float32)
    left_proj = project(normed, w_left, b_left, mask_f32)
    right_proj = project(normed, w_right, b_right, mask_f32)
    right_f32 = right_proj.astype(jnp.float32)
    w_out3 = w_out.astype(jnp.float32).reshape(CH, CH, CZ)
    left_blocks = jnp.moveaxis(left_proj.astype(jnp.float32).reshape(S, N // ROW_BLOCK, ROW_BLOCK, CH), 1, 0)

    def row_block(left_blk):
        outer_blk = jnp.einsum('sic,sjd->icjd', left_blk, right_f32).astype(jnp.bfloat16)
        return jnp.einsum('icjd,cde->ije', outer_blk.astype(jnp.float32), w_out3)

    proj_sum = lax.map(row_block, left_blocks).reshape(N, N, CZ)
    pair_count = jnp.dot(mask_f32.T, mask_f32)
    pair_out = pair_act + (proj_sum + b_out.astype(jnp.float32)) / (1e-3 + pair_count)[:, :, None]
    return pair_out, msa_act
```

```python
import functools
import jax
import jax.numpy as jnp
from jax import lax
from jax.experimental import pallas as pl
from jax.experimental.pallas import tpu as pltpu
from jax.sharding import PartitionSpec as P

F32 = jnp.float32
BF16 = jnp.bfloat16
LAG1 = 1
LAG2 = 2


def iota(shape, dim):
    return lax.broadcasted_iota(jnp.int32, shape, dim)


def onehot(cond):
    return jnp.where(cond, 1.0, 0.0).astype(BF16)


def dot(a, b):
    return jnp.dot(a, b, preferred_element_type=F32)


def dot_nt(a, b):
    return lax.dot_general(a, b, (((1,), (1,)), ((), ())), preferred_element_type=F32)


def dot_tn(a, b):
    return lax.dot_general(a, b, (((0,), (0,)), ((), ())), preferred_element_type=F32)


def kernel(dims, m_hbm, mask_hbm, z_hbm, vecs, waT, wbT, wo, zo_hbm, mo_hbm,
           mT, mkv, zv, xT, wbig, bbb, mkT, acat, bT, wblk, lbuf, rp, rq, sp, sq, rc, mr, tbuf, ov,
           sem_in, sem_out, bs_own, bs_fwd, bs_rel, b_recv, ms_dir, ms_opp, ms_fwd, ms_rel, m_recv, mf_recv, m_prel,
           y1s, y1r, y2s, y2r):
    n_y, n_d = dims
    n_x = n_d // 2
    yy = lax.axis_index("seq")
    dd = lax.axis_index("dap")
    xx = dd // 2
    cc = dd % 2
    x_r = (xx + 1) % n_x
    x_l = (xx + n_x - 1) % n_x
    x_o = (xx + 2) % n_x
    right, left, mate = 2 * x_r + cc, 2 * x_l + cc, 2 * xx + 1 - cc
    par = yy % 2
    y_a = yy + 1 - 2 * par
    y_b = (yy + n_y - 1 + 2 * par) % n_y
    n_i, n_ch, s_loc = mT.shape
    s_all, n_j = mkv.shape
    c_hid = waT.shape[0]
    half = n_i // 2
    hrows = half * c_hid
    s_chip = s_loc // n_x
    s_dev = s_loc // n_d

    def to_dap(idx):
        return dict(device_id={"dap": idx}, device_id_type=pl.DeviceIdType.MESH)

    def to_seq(idx):
        return dict(device_id={"seq": idx}, device_id_type=pl.DeviceIdType.MESH)

    in_m = pltpu.make_async_copy(m_hbm, mT, sem_in.at[0])
    in_mask = pltpu.make_async_copy(mask_hbm, mkv, sem_in.at[1])
    in_z = pltpu.make_async_copy(z_hbm, zv, sem_in.at[2])
    in_m.start()
    in_mask.start()
    in_z.start()

    barrier = pltpu.get_barrier_semaphore()
    for nb in (right, left, mate):
        pl.semaphore_signal(barrier, inc=1, **to_dap(nb))
    for nb in (y_a, y_b):
        pl.semaphore_signal(barrier, inc=1, **to_seq(nb))

    def remote(src, dst, ssem, rsem, to):
        return pltpu.make_async_remote_copy(src_ref=src, dst_ref=dst, send_sem=ssem, recv_sem=rsem, **to)

    def b_to(src_u, src_p, dst_u, dst_p, ssem, nb):
        return remote(bT.at[src_u, src_p], bT.at[dst_u, dst_p], ssem, b_recv.at[dst_u, dst_p], to_dap(nb))

    b_r0 = b_to(0, 0, 2, 0, bs_own.at[0], right)
    b_r1 = b_to(0, 1, 4, 0, bs_own.at[1], right)
    b_l1 = b_to(0, 1, 2, 1, bs_own.at[2], left)
    b_l0 = b_to(0, 0, 4, 1, bs_own.at[3], left)
    b_fr = b_to(2, 0, 6, 0, bs_fwd.at[0], right)
    b_fl = b_to(2, 1, 6, 1, bs_fwd.at[1], left)

    def b_rel(u, p):
        return b_to(u, p, u + 1, p, bs_rel.at[u, p], mate)

    def b_wait(u, p):
        b_to(u, p, u, p, bs_rel.at[u, p], mate).wait_recv()

    def lanes_of(xc):
        return pl.ds(pl.multiple_of(xc * s_chip, s_chip), s_chip)

    d_right, d_left, d_opp = 2 * x_r + cc, 2 * x_l + cc, 2 * x_o + cc
    up, lo = pl.ds(0, half), pl.ds(half, half)
    m_or = remote(mT.at[up, :, lanes_of(x_o)], tbuf.at[0], ms_opp.at[0], mf_recv.at[0], to_dap(right))
    m_ol = remote(mT.at[lo, :, lanes_of(x_o)], tbuf.at[1], ms_opp.at[1], mf_recv.at[1], to_dap(left))
    m_dr = remote(mT.at[:, :, lanes_of(x_r)], mr.at[dd], ms_dir.at[0], m_recv.at[0], to_dap(right))
    m_dl = remote(mT.at[:, :, lanes_of(x_l)], mr.at[dd], ms_dir.at[1], m_recv.at[1], to_dap(left))
    m_fr = remote(tbuf.at[0], mr.at[d_left, up], ms_fwd.at[0], m_recv.at[2], to_dap(right))
    m_fl = remote(tbuf.at[1], mr.at[d_right, lo], ms_fwd.at[1], m_recv.at[3], to_dap(left))
    m_p0 = remote(mT.at[:, :, lanes_of(xx)], mr.at[dd], ms_rel.at[0], m_prel.at[0], to_dap(mate))
    m_p1 = remote(mr.at[d_left], mr.at[d_left], ms_rel.at[1], m_prel.at[1], to_dap(mate))
    m_p2 = remote(mr.at[d_right], mr.at[d_right], ms_rel.at[2], m_prel.at[2], to_dap(mate))
    m_p3 = remote(mr.at[d_opp], mr.at[d_opp], ms_rel.at[3], m_prel.at[3], to_dap(mate))
    m_self = pltpu.make_async_copy(m_hbm.at[:, :, lanes_of(xx)], mr.at[dd], sem_in.at[3])

    def m_wait(ref, sem):
        remote(ref, ref, ms_rel.at[0], sem, to_dap(mate)).wait_recv()

    rowc = iota((hrows, c_hid), 0) // half
    rep_b = onehot(rowc == iota((hrows, c_hid), 1))
    gam, bet = vecs[0:1, 0:n_ch], vecs[1:2, 0:n_ch]
    ones_ch = jnp.ones((n_ch, 128), BF16)
    eye_ch = iota((n_ch, n_ch), 0) == iota((n_ch, n_ch), 1)
    gcol = dot(jnp.where(eye_ch, jnp.broadcast_to(gam, (n_ch, n_ch)), 0.0).astype(BF16), ones_ch)[:, 0:1]
    bcol = dot(jnp.where(eye_ch, jnp.broadcast_to(bet, (n_ch, n_ch)), 0.0).astype(BF16), ones_ch)[:, 0:1]
    eye_h = iota((c_hid, c_hid), 0) == iota((c_hid, c_hid), 1)
    bl = jnp.where(eye_h, jnp.broadcast_to(vecs[2:3, 0:c_hid], (c_hid, c_hid)), 0.0).astype(BF16)
    br = jnp.where(eye_h, jnp.broadcast_to(vecs[3:4, 0:c_hid], (c_hid, c_hid)), 0.0).astype(BF16)
    ones_h = jnp.ones((c_hid, 128), BF16)
    kb = half * n_ch
    tile_b = onehot(iota((n_ch, kb), 1) % n_ch == iota((n_ch, kb), 0))
    wrep = dot(rep_b, wbT[...]).astype(BF16)
    wide = dot(wrep, tile_b)
    keep = iota((hrows, kb), 0) % half == iota((hrows, kb), 1) // n_ch
    wbig[...] = jnp.where(keep, wide, 0.0).astype(BF16)
    brep = dot(dot(rep_b, br).astype(BF16), ones_h)[:, 0:n_i]
    bj = iota((hrows, n_i), 0) % half
    for h in range(2):
        bbb[h] = jnp.where(iota((hrows, n_i), 1) == bj + h * half, brep, 0.0).astype(BF16)

    in_mask.wait()
    selT = onehot(iota((n_i, n_j), 1) == iota((n_i, n_j), 0) + dd * n_i)
    mloc = mkv[pl.ds(pl.multiple_of(yy * s_loc, s_loc), s_loc), :].astype(F32).astype(BF16)
    mkT[...] = dot_nt(selT, mloc)

    in_m.wait()
    pl.semaphore_wait(barrier, 5)
    m_or.start()
    m_ol.start()
    m_p0.start()
    m_self.start()

    def norm_row(r, carry):
        act = mT[r].astype(F32)
        mean = jnp.sum(act, axis=0, keepdims=True) * (1.0 / n_ch)
        cen = act - mean
        var = jnp.sum(cen * cen, axis=0, keepdims=True) * (1.0 / n_ch)
        nrm = cen * lax.rsqrt(var + 1e-5)
        val = (nrm * gcol + bcol).astype(BF16).astype(F32) * mkT[pl.ds(r, 1), :]
        xT[pl.ds(pl.multiple_of(r * n_ch, n_ch), n_ch), :] = val.astype(BF16)
        return carry

    mk16 = mkT[...].astype(BF16)
    for h in range(2):
        lax.fori_loop(h * half, (h + 1) * half, norm_row, 0)
        for q in range(2):
            rows = slice(q * hrows // 2, (q + 1) * hrows // 2)
            acc = dot(wbig[rows, :], xT[h * kb:(h + 1) * kb, :]) + dot(bbb[h, rows, :], mk16)
            bT[0, h, rows, :] = acc.astype(BF16)
        if h == 0:
            b_r0.start()
        else:
            b_l1.start()
            b_l0.start()
            b_r1.start()
        b_rel(0, h).start()

    ga = 128 // c_hid
    ra = onehot(iota((128, c_hid), 0) % c_hid == iota((128, c_hid), 1))
    ka = ga * n_ch
    wa_rep = dot(dot(ra, waT[...]).astype(BF16), onehot(iota((n_ch, ka), 1) % n_ch == iota((n_ch, ka), 0)))
    wa4 = jnp.where(iota((128, ka), 0) // c_hid == iota((128, ka), 1) // n_ch, wa_rep, 0.0).astype(BF16)
    ba_rep = dot(dot(ra, bl).astype(BF16), ones_h)[:, 0:n_i]
    n_g = n_i // ga
    for g in range(n_g):
        bag = jnp.where(iota((128, n_i), 1) == iota((128, n_i), 0) // c_hid + ga * g, ba_rep, 0.0).astype(BF16)
        at = dot(wa4, xT[g * ka:(g + 1) * ka, :]) + dot(bag, mk16)
        acat[g // 2, :, (g % 2) * 128:(g % 2 + 1) * 128] = at.T.astype(BF16)

    n_e = wo.shape[1]
    wblk[...] = jnp.zeros_like(wblk)

    def place(dc, carry):
        r0, c0 = iota((128, c_hid * c_hid), 0), iota((128, c_hid * c_hid), 1)
        perm = onehot(c0 == (r0 % c_hid) * c_hid + dc * ga + r0 // c_hid)
        wp = dot(perm, wo[...]).astype(BF16)
        for k in range(ga):
            for i4 in range(ga):
                row = pl.multiple_of((dc * ga + k) * 128 + i4 * c_hid, c_hid)
                wblk[pl.ds(row, c_hid), i4 * n_e:(i4 + 1) * n_e] = wp[k * c_hid:(k + 1) * c_hid, :]
        return carry

    lax.fori_loop(0, c_hid // ga, place, 0)

    def pair_counts():
        sel = onehot(iota((n_j, 128), 0) == iota((n_j, 128), 1) + dd * n_i)
        rc[...] = jnp.zeros_like(rc)

        def add(k, carry):
            mk = mkv[pl.ds(pl.multiple_of(k * s_loc, s_loc), s_loc), :].astype(F32).astype(BF16)
            rc[...] += dot_tn(mk, dot(mk, sel).astype(BF16))
            return carry

        lax.fori_loop(0, s_all // s_loc, add, 0)
        rc[...] = 1.0 / (1e-3 + rc[...])

    def compute(t):
        def outer(q, carry):
            h, n = q // 4, q % 4
            acc = dot(bT[t, h], acat[n]).astype(BF16)
            for d in range(c_hid):
                for gg in range(2):
                    lbuf[(2 * n + gg) * 2 + h, :, d * 128:(d + 1) * 128] = acc[d * half:(d + 1) * half, gg * 128:(gg + 1) * 128]
            return carry

        lax.fori_loop(0, 8, outer, 0)
        for nn in range(2):
            cols = slice(nn * 256, (nn + 1) * 256)
            res = dot(lbuf[...].reshape(n_g * n_i, c_hid * 128), wblk[:, cols]).astype(BF16)
            for g in range(n_g):
                for k in range(2):
                    i = ga * g + 2 * nn + k
                    rp[t, i // half, i % half] = res[g * n_i:(g + 1) * n_i, k * 128:(k + 1) * 128]

    def y1(t, f):
        return remote(rp.at[t, f], rq.at[t, f], y1s.at[t, f], y1r.at[t, f], to_seq(y_a if f == 0 else y_b))

    def y2(t, f):
        return remote(sp.at[t, f], sq.at[t, f], y2s.at[t, f], y2r.at[t, f], to_seq(y_b if f == 0 else y_a))

    def j_of(t, p):
        u = t // 2
        off = jnp.where(u == 0, 0, jnp.where(u == 3, 2, n_x - 1 if p == 0 else 1))
        core = jnp.where(t % 2 == 0, cc, 1 - cc)
        hh = jnp.where(u == 2, 1 - p, p)
        return pl.multiple_of((2 * ((xx + off) % n_x) + core) * n_i + hh * half, half)

    def finish(t):
        for f in range(2):
            y2(t, f).wait_recv()
        for p in range(2):
            j0 = j_of(t, p)
            rcp = rc[pl.ds(j0, half), :]
            for i in range(n_i):
                rows = slice(p * half, (p + 1) * half)
                tot = sp[t, i // half, i % half, rows, :].astype(F32) + sq[t, i // half, i % half, rows, :].astype(F32)
                upd = (tot + vecs[4:5, :]) * jnp.broadcast_to(rcp[:, i:i + 1], (half, n_e))
                zv[i, pl.ds(j0, half), :] += upd

    def step(t, carry):
        @pl.when(t == 1)
        def _():
            b_wait(1, 0)
            b_wait(1, 1)

        @pl.when(t == 2)
        def _():
            b_wait(2, 0)
            b_fr.start()
            b_rel(2, 0).start()
            b_wait(2, 1)
            b_fl.start()
            b_rel(2, 1).start()
            m_wait(tbuf.at[0], mf_recv.at[0])
            m_fr.start()
            m_wait(tbuf.at[1], mf_recv.at[1])
            m_fl.start()
            m_dr.start()
            m_dl.start()

        @pl.when(t == 3)
        def _():
            b_wait(3, 0)
            b_wait(3, 1)

        @pl.when(t == 4)
        def _():
            b_wait(4, 0)
            b_rel(4, 0).start()
            b_wait(4, 1)
            b_rel(4, 1).start()

        @pl.when(t == 5)
        def _():
            b_wait(5, 0)
            b_wait(5, 1)

        @pl.when(t == 6)
        def _():
            b_wait(6, 0)
            b_rel(6, 0).start()
            b_wait(6, 1)
            b_rel(6, 1).start()

        @pl.when(t == 7)
        def _():
            b_wait(7, 0)
            b_wait(7, 1)

        @pl.when(t < 8)
        def _():
            compute(t)
            for f in range(2):
                y1(t, f).start()

        @pl.when(t == 1)
        def _():
            in_z.wait()
            pair_counts()

        @pl.when(jnp.logical_and(t >= LAG1, t < 8 + LAG1))
        def _():
            v = t - LAG1
            for f in range(2):
                y1(v, f).wait_recv()

                def add(i, carry):
                    tot = rp[v, f, i].astype(F32) + rq[v, f, i].astype(F32)
                    sp[v, f, i] = tot.astype(BF16)
                    return carry

                lax.fori_loop(0, half, add, 0)
                y2(v, f).start()

        @pl.when(t >= LAG2)
        def _():
            finish(t - LAG2)

        return carry

    lax.fori_loop(0, 8 + LAG2, step, 0)
    out_z = pltpu.make_async_copy(zv, zo_hbm, sem_out.at[0])
    out_z.start()

    m_wait(mr.at[d_opp, up], m_recv.at[2])
    m_wait(mr.at[d_opp, lo], m_recv.at[3])
    m_p3.start()
    m_wait(mr.at[d_left], m_recv.at[0])
    m_p1.start()
    m_wait(mr.at[d_right], m_recv.at[1])
    m_p2.start()
    m_self.wait()
    for k in range(4):
        m_wait(mr.at[0], m_prel.at[k])

    per = 128 // n_i

    def regroup(q, carry):
        k, c0 = q // (n_ch // 16), q % (n_ch // 16)
        blk = mr[pl.ds(per * k, per), :, pl.ds(pl.multiple_of(c0 * 16, 16), 16), :].astype(F32)
        blk = jnp.transpose(blk.reshape(128, 16, s_chip), (1, 0, 2))
        blk = jnp.transpose(blk, (0, 2, 1))
        mine = jnp.where(cc == 0, blk[:, 0:s_dev, :], blk[:, s_dev:, :])
        ov[k, :, pl.ds(pl.multiple_of(c0 * 16, 16), 16), :] = jnp.transpose(mine, (1, 0, 2)).astype(BF16)
        return carry

    lax.fori_loop(0, n_d // per * (n_ch // 16), regroup, 0)
    outs = [pltpu.make_async_copy(ov.at[k], mo_hbm.at[:, :, k * 128:(k + 1) * 128], sem_out.at[1 + k]) for k in range(n_d // per)]
    for o in outs:
        o.start()

    for cp in (b_r0, b_r1, b_l1, b_l0, b_fr, b_fl, m_or, m_ol, m_dr, m_dl, m_fr, m_fl, m_p0, m_p1, m_p2, m_p3):
        cp.wait_send()
    for u in (0, 2, 4, 6):
        for p in range(2):
            b_rel(u, p).wait_send()

    def drain(t, carry):
        for f in range(2):
            y1(t, f).wait_send()
            y2(t, f).wait_send()
        return carry

    lax.fori_loop(0, 8, drain, 0)
    out_z.wait()
    for o in outs:
        o.wait()


def solution(mesh):
    n_y, n_d = mesh.shape["seq"], mesh.shape["dap"]
    rep = P()
    in_specs = (P(("data", "seq"), "dap", None), P("data", None), P(("data", "dap"), None, None)) + (rep,) * 8
    out_specs = (P(("data", "dap"), None, None), P(("data", "seq", "dap"), None, None))

    def local_fn(m, mask, z, gamma, beta, w_l, b_l, w_r, b_r, w_o, b_o):
        s_loc, n_i, n_ch = m.shape
        s_all, n_j = mask.shape
        n_e = w_o.shape[1]
        c_hid = w_l.shape[1]
        half = n_i // 2
        hrows = half * c_hid
        s_dev = s_loc // n_d
        vecs = jnp.stack([jnp.pad(v.astype(F32), (0, n_e - v.shape[0])) for v in (gamma, beta, b_l, b_r, b_o)])
        any_spec = pl.BlockSpec(memory_space=pl.ANY)
        vm = pl.BlockSpec(memory_space=pltpu.VMEM)
        dma = pltpu.SemaphoreType.DMA
        ysh = (8, 2, half, n_i, n_e)
        z_out, m_out = pl.pallas_call(
            functools.partial(kernel, (n_y, n_d)),
            out_shape=(jax.ShapeDtypeStruct(z.shape, F32), jax.ShapeDtypeStruct((s_dev, n_ch, n_j), BF16)),
            in_specs=[any_spec] * 3 + [vm] * 4,
            out_specs=(any_spec, any_spec),
            scratch_shapes=[
                pltpu.VMEM((n_i, n_ch, s_loc), BF16),
                pltpu.VMEM((s_all, n_j), jnp.int32),
                pltpu.VMEM(z.shape, F32),
                pltpu.VMEM((n_i * n_ch, s_loc), BF16),
                pltpu.VMEM((hrows, half * n_ch), BF16),
                pltpu.VMEM((2, hrows, n_i), BF16),
                pltpu.VMEM((n_i, s_loc), F32),
                pltpu.VMEM((4, s_loc, 256), BF16),
                pltpu.VMEM((8, 2, hrows, s_loc), BF16),
                pltpu.VMEM((c_hid * 128, 4 * n_e), BF16),
                pltpu.VMEM((16, half, c_hid * 128), BF16),
                pltpu.VMEM(ysh, BF16),
                pltpu.VMEM(ysh, BF16),
                pltpu.VMEM(ysh, BF16),
                pltpu.VMEM(ysh, BF16),
                pltpu.VMEM((n_j, 128), F32),
                pltpu.VMEM((n_d, n_i, n_ch, s_loc * 2 // n_d), BF16),
                pltpu.VMEM((2, half, n_ch, s_loc * 2 // n_d), BF16),
                pltpu.VMEM((n_j // 128, s_dev, n_ch, 128), BF16),
                dma((4,)), dma((3,)), dma((4,)), dma((2,)), dma((8, 2)), dma((8, 2)),
                dma((2,)), dma((2,)), dma((2,)), dma((4,)), dma((4,)), dma((2,)), dma((4,)),
                dma((8, 2)), dma((8, 2)), dma((8, 2)), dma((8, 2)),
            ],
            compiler_params=pltpu.CompilerParams(collective_id=0, has_side_effects=True, vmem_limit_bytes=63 * 2**20),
            name="opm",
        )(jnp.transpose(m, (1, 2, 0)), mask, z, vecs, w_l.T, w_r.T, w_o)
        return z_out, jnp.transpose(m_out, (0, 2, 1))

    return jax.shard_map(local_fn, mesh=mesh, in_specs=in_specs, out_specs=out_specs, check_vma=False)
```

```python
import functools
import jax
import jax.numpy as jnp
from jax import lax
from jax.experimental import pallas as pl
from jax.experimental.pallas import tpu as pltpu
from jax.sharding import PartitionSpec as P

F32 = jnp.float32
BF16 = jnp.bfloat16
VM_LIM = 56
LAG1 = 1
LAG2 = 2


def iota(shape, dim):
    return lax.broadcasted_iota(jnp.int32, shape, dim)


def onehot(cond):
    return jnp.where(cond, 1.0, 0.0).astype(BF16)


def dot(a, b):
    return jnp.dot(a, b, preferred_element_type=F32)


def dot_nt(a, b):
    return lax.dot_general(a, b, (((1,), (1,)), ((), ())), preferred_element_type=F32)


def dot_tn(a, b):
    return lax.dot_general(a, b, (((0,), (0,)), ((), ())), preferred_element_type=F32)


def kernel(dims, m_hbm, mask_hbm, z_hbm, gam, bet, bias_l, bias_r, bias_o, waT, wbT, wo, zv, ov,
           mT, mkv, mkl, xT, wbig, bbb, mkT, acat, bT, wblk, lbuf, rp, rq, sp, sq, rc, mr, tbuf,
           sem_in, bs_own, bs_fwd, bs_rel, b_recv, ms_dir, ms_opp, ms_fwd, ms_rel, m_recv, mf_recv, m_prel,
           y1s, y1r, y2s, y2r):
    n_y, n_d = dims
    n_x = n_d // 2
    yy = lax.axis_index("seq")
    dd = lax.axis_index("dap")
    xx = dd // 2
    cc = dd % 2
    x_r = (xx + 1) % n_x
    x_l = (xx + n_x - 1) % n_x
    x_o = (xx + 2) % n_x
    right, left, mate = 2 * x_r + cc, 2 * x_l + cc, 2 * xx + 1 - cc
    par = yy % 2
    y_a = yy + 1 - 2 * par
    y_b = (yy + n_y - 1 + 2 * par) % n_y
    n_i, n_ch, s_loc = mT.shape
    s_all, n_j = mkv.shape
    c_hid = waT.shape[0]
    half = n_i // 2
    hrows = half * c_hid
    s_chip = s_loc // n_x
    s_dev = s_loc // n_d

    def to_dap(idx):
        return dict(device_id={"dap": idx}, device_id_type=pl.DeviceIdType.MESH)

    def to_seq(idx):
        return dict(device_id={"seq": idx}, device_id_type=pl.DeviceIdType.MESH)

    in_m = pltpu.make_async_copy(m_hbm, mT, sem_in.at[0])
    mine_rows = pl.ds(pl.multiple_of(yy * s_loc, s_loc), s_loc)
    in_mloc = pltpu.make_async_copy(mask_hbm.at[mine_rows], mkl, sem_in.at[4])
    in_mask = pltpu.make_async_copy(mask_hbm, mkv, sem_in.at[1])
    in_z = pltpu.make_async_copy(z_hbm, zv, sem_in.at[2])
    in_mloc.start()
    in_m.start()

    barrier = pltpu.get_barrier_semaphore()
    for nb in (right, left, mate):
        pl.semaphore_signal(barrier, inc=1, **to_dap(nb))
    for nb in (y_a, y_b):
        pl.semaphore_signal(barrier, inc=1, **to_seq(nb))

    def remote(src, dst, ssem, rsem, to):
        return pltpu.make_async_remote_copy(src_ref=src, dst_ref=dst, send_sem=ssem, recv_sem=rsem, **to)

    def b_to(src_u, src_p, dst_u, dst_p, ssem, nb):
        return remote(bT.at[src_u, src_p], bT.at[dst_u, dst_p], ssem, b_recv.at[dst_u, dst_p], to_dap(nb))

    b_r0 = b_to(0, 0, 2, 0, bs_own.at[0], right)
    b_r1 = b_to(0, 1, 4, 0, bs_own.at[1], right)
    b_l1 = b_to(0, 1, 2, 1, bs_own.at[2], left)
    b_l0 = b_to(0, 0, 4, 1, bs_own.at[3], left)
    b_fr = b_to(2, 0, 6, 0, bs_fwd.at[0], right)
    b_fl = b_to(2, 1, 6, 1, bs_fwd.at[1], left)

    def b_rel(u, p):
        return b_to(u, p, u + 1, p, bs_rel.at[u, p], mate)

    def b_wait(u, p):
        b_to(u, p, u, p, bs_rel.at[u, p], mate).wait_recv()

    def lanes_of(xc):
        return pl.ds(pl.multiple_of(xc * s_chip, s_chip), s_chip)

    d_right, d_left, d_opp = 2 * x_r + cc, 2 * x_l + cc, 2 * x_o + cc
    up, lo = pl.ds(0, half), pl.ds(half, half)
    m_or = remote(m_hbm.at[up, :, lanes_of(x_o)], tbuf.at[0], ms_opp.at[0], mf_recv.at[0], to_dap(right))
    m_ol = remote(m_hbm.at[lo, :, lanes_of(x_o)], tbuf.at[1], ms_opp.at[1], mf_recv.at[1], to_dap(left))
    m_dr = remote(m_hbm.at[:, :, lanes_of(x_r)], mr.at[dd], ms_dir.at[0], m_recv.at[0], to_dap(right))
    first, rest = pl.ds(0, n_i // 4), pl.ds(n_i // 4, n_i - n_i // 4)
    m_dl0 = remote(m_hbm.at[first, :, lanes_of(x_l)], mr.at[dd, first], ms_dir.at[2], m_recv.at[4], to_dap(left))
    m_dl = remote(m_hbm.at[rest, :, lanes_of(x_l)], mr.at[dd, rest], ms_dir.at[1], m_recv.at[1], to_dap(left))
    m_fr = remote(tbuf.at[0], mr.at[d_left, up], ms_fwd.at[0], m_recv.at[2], to_dap(right))
    m_fl = remote(tbuf.at[1], mr.at[d_right, lo], ms_fwd.at[1], m_recv.at[3], to_dap(left))
    m_p0 = remote(m_hbm.at[:, :, lanes_of(xx)], mr.at[dd], ms_rel.at[0], m_prel.at[0], to_dap(mate))
    m_p1 = remote(mr.at[d_left], mr.at[d_left], ms_rel.at[1], m_prel.at[1], to_dap(mate))
    m_p2 = remote(mr.at[d_right], mr.at[d_right], ms_rel.at[2], m_prel.at[2], to_dap(mate))
    m_p3 = remote(mr.at[d_opp], mr.at[d_opp], ms_rel.at[3], m_prel.at[3], to_dap(mate))
    m_self = pltpu.make_async_copy(m_hbm.at[:, :, lanes_of(xx)], mr.at[dd], sem_in.at[3])

    def m_wait(ref, sem):
        remote(ref, ref, ms_rel.at[0], sem, to_dap(mate)).wait_recv()

    pl.semaphore_wait(barrier, 5)
    m_or.start()
    m_ol.start()
    m_dl0.start()
    m_p0.start()

    def column(row, n, wide):
        eye = iota((n, n), 0) == iota((n, n), 1)
        diag = jnp.where(eye, jnp.broadcast_to(row, (n, n)), 0.0).astype(BF16)
        return dot(diag, jnp.ones((n, wide), BF16))

    lw = s_loc // 2
    gcol = column(gam[...].astype(F32), n_ch, lw)
    bcol = column(bet[...].astype(F32), n_ch, lw)
    blc = column(bias_l[...].astype(F32), c_hid, 128)
    brc = column(bias_r[...].astype(F32), c_hid, 128)
    kb = half * n_ch
    wide = dot(wbT[...], onehot((iota((n_ch, kb), 1) & (n_ch - 1)) == iota((n_ch, kb), 0)))
    keep = iota((half, kb), 0) == iota((half, kb), 1) // n_ch
    lane_i = iota((half, n_i), 1) - iota((half, n_i), 0)
    for d in range(c_hid):
        rows = slice(d * half, (d + 1) * half)
        wbig[rows, :] = jnp.where(keep, jnp.broadcast_to(wide[d:d + 1, :], (half, kb)), 0.0).astype(BF16)
        bias = jnp.broadcast_to(brc[d:d + 1, 0:n_i], (half, n_i))
        for h in range(2):
            bbb[h, rows, :] = jnp.where(lane_i == h * half, bias, 0.0).astype(BF16)

    in_mloc.wait()
    selT = onehot(iota((n_i, n_j), 1) == iota((n_i, n_j), 0) + dd * n_i)
    mkT[...] = dot_nt(selT, mkl[...].astype(F32).astype(BF16))
    in_m.wait()

    ga = 128 // c_hid
    n_e = wo.shape[1]
    pos = iota((128, c_hid * c_hid), 0)
    want = (pos & (c_hid - 1)) * c_hid + pos // c_hid
    gap = iota((128, c_hid * c_hid), 1) - want

    def place(dc, carry):
        wp = dot(onehot(gap == dc * ga), wo[...]).astype(BF16)
        for k in range(ga):
            for i4 in range(ga):
                row = pl.multiple_of((dc * ga + k) * 128 + i4 * c_hid, c_hid)
                wblk[pl.ds(row, c_hid), i4 * n_e:(i4 + 1) * n_e] = wp[k * c_hid:(k + 1) * c_hid, :]
        return carry

    def norm_row(r, carry):
        for q in range(2):
            lanes = slice(q * lw, (q + 1) * lw)
            act = mT[r, :, lanes].astype(F32)
            mean = jnp.sum(act, axis=0, keepdims=True) * (1.0 / n_ch)
            cen = act - mean
            var = jnp.sum(cen * cen, axis=0, keepdims=True) * (1.0 / n_ch)
            nrm = cen * lax.rsqrt(var + 1e-5)
            val = (nrm * gcol + bcol).astype(BF16) * mkT[pl.ds(r, 1), lanes].astype(BF16)
            xT[pl.ds(pl.multiple_of(r * n_ch, n_ch), n_ch), lanes] = val
        return carry

    mk16 = mkT[...].astype(BF16)
    for h in range(2):
        lax.fori_loop(h * half, (h + 1) * half, norm_row, 0, unroll=2)
        acc = dot(wbig[...], xT[h * kb:(h + 1) * kb, :]) + dot(bbb[h], mk16)
        bT[0, h] = acc.astype(BF16)
        if h == 0:
            b_r0.start()
        else:
            b_l1.start()
            b_l0.start()
            b_r1.start()
        b_rel(0, h).start()
    m_self.start()
    in_mask.start()
    in_z.start()

    ka = ga * n_ch
    ra = onehot((iota((128, c_hid), 0) & (c_hid - 1)) == iota((128, c_hid), 1))
    wa_rep = dot(dot(ra, waT[...]).astype(BF16), onehot((iota((n_ch, ka), 1) & (n_ch - 1)) == iota((n_ch, ka), 0)))
    wa4 = jnp.where(iota((128, ka), 0) // c_hid == iota((128, ka), 1) // n_ch, wa_rep, 0.0).astype(BF16)
    ba_rep = dot(ra, blc.astype(BF16))[:, 0:n_i]
    lane_a = iota((128, n_i), 1) - iota((128, n_i), 0) // c_hid
    n_g = n_i // ga
    for g in range(n_g):
        bag = jnp.where(lane_a == ga * g, ba_rep, 0.0).astype(BF16)
        at = dot(wa4, xT[g * ka:(g + 1) * ka, :]) + dot(bag, mk16)
        acat[g // 2, :, (g % 2) * 128:(g % 2 + 1) * 128] = at.T.astype(BF16)

    wblk[...] = jnp.zeros_like(wblk)
    lax.fori_loop(0, c_hid // ga, place, 0, unroll=4)

    def pair_counts():
        sel = onehot(iota((n_j, 128), 0) == iota((n_j, 128), 1) + dd * n_i)
        rc[...] = jnp.zeros_like(rc)

        def add(k, carry):
            mk = mkv[pl.ds(pl.multiple_of(k * s_loc, s_loc), s_loc), :].astype(F32).astype(BF16)
            rc[...] += dot_tn(mk, dot(mk, sel).astype(BF16))
            return carry

        lax.fori_loop(0, s_all // s_loc, add, 0, unroll=2)
        rc[...] = 1.0 / (1e-3 + rc[...])

    def compute(t):
        lhs = bT[t].reshape(2 * hrows, s_loc)
        for n in range(4):
            acc = dot(lhs, acat[n]).astype(BF16)
            for h in range(2):
                for d in range(c_hid):
                    row = (h * c_hid + d) * half
                    for gg in range(2):
                        lbuf[(2 * n + gg) * 2 + h, :, d * 128:(d + 1) * 128] = acc[row:row + half, gg * 128:(gg + 1) * 128]
        for nn in range(2):
            cols = slice(nn * 256, (nn + 1) * 256)
            res = dot(lbuf[...].reshape(n_g * n_i, c_hid * 128), wblk[:, cols]).astype(BF16)
            for g in range(n_g):
                for k in range(2):
                    i = ga * g + 2 * nn + k
                    rp[t, i // half, i % half] = res[g * n_i:(g + 1) * n_i, k * 128:(k + 1) * 128]

    def y1(t, f):
        return remote(rp.at[t, f], rq.at[t, f], y1s.at[t, f], y1r.at[t, f], to_seq(y_a if f == 0 else y_b))

    def y2(t, f):
        return remote(sp.at[t, f], sq.at[t, f], y2s.at[t, f], y2r.at[t, f], to_seq(y_b if f == 0 else y_a))

    def j_of(t, p):
        u = t // 2
        off = jnp.where(u == 0, 0, jnp.where(u == 3, 2, n_x - 1 if p == 0 else 1))
        core = jnp.where(t % 2 == 0, cc, 1 - cc)
        hh = jnp.where(u == 2, 1 - p, p)
        return pl.multiple_of((2 * ((xx + off) % n_x) + core) * n_i + hh * half, half)

    def finish(t):
        bo = bias_o[...].astype(F32)
        for f in range(2):
            y2(t, f).wait_recv()
        for p in range(2):
            j0 = j_of(t, p)
            rcp = rc[pl.ds(j0, half), :]
            for i in range(n_i):
                rows = slice(p * half, (p + 1) * half)
                tot = sp[t, i // half, i % half, rows, :].astype(F32) + sq[t, i // half, i % half, rows, :].astype(F32)
                upd = (tot + bo) * jnp.broadcast_to(rcp[:, i:i + 1], (half, n_e))
                zv[i, pl.ds(j0, half), :] += upd

    per = 128 // n_i

    def regroup(k):
        def part(c0, carry):
            chs = pl.ds(pl.multiple_of(c0 * 16, 16), 16)
            blk = mr[pl.ds(per * k, per), :, chs, :].astype(F32)
            blk = jnp.transpose(blk.reshape(128, 16, s_chip), (1, 0, 2))
            blk = jnp.transpose(blk, (0, 2, 1))
            mine = jnp.where(cc == 0, blk[:, 0:s_dev, :], blk[:, s_dev:, :])
            ov[:, chs, pl.ds(pl.multiple_of(k * 128, 128), 128)] = jnp.transpose(mine, (1, 0, 2)).astype(BF16)
            return carry

        lax.fori_loop(0, n_ch // 16, part, 0)

    def step(t, carry):
        @pl.when(t == 1)
        def _():
            b_wait(1, 0)
            b_wait(1, 1)

        @pl.when(t == 2)
        def _():
            in_mask.wait()
            in_z.wait()
            pair_counts()
            b_wait(2, 0)
            b_fr.start()
            b_rel(2, 0).start()
            b_wait(2, 1)
            b_fl.start()
            b_rel(2, 1).start()
            m_dr.start()
            m_dl.start()
            m_wait(tbuf.at[0], mf_recv.at[0])
            m_fr.start()
            m_wait(tbuf.at[1], mf_recv.at[1])
            m_fl.start()

        @pl.when(t == 3)
        def _():
            b_wait(3, 0)
            b_wait(3, 1)

        @pl.when(t == 4)
        def _():
            b_wait(4, 0)
            b_rel(4, 0).start()
            b_wait(4, 1)
            b_rel(4, 1).start()

        @pl.when(t == 5)
        def _():
            b_wait(5, 0)
            b_wait(5, 1)

        @pl.when(t == 6)
        def _():
            b_wait(6, 0)
            b_rel(6, 0).start()
            b_wait(6, 1)
            b_rel(6, 1).start()

        @pl.when(t == 7)
        def _():
            b_wait(7, 0)
            b_wait(7, 1)

        @pl.when(t < 8)
        def _():
            compute(t)
            for f in range(2):
                y1(t, f).start()

        @pl.when(jnp.logical_and(t >= LAG1, t < 8 + LAG1))
        def _():
            v = t - LAG1
            for f in range(2):
                y1(v, f).wait_recv()

                def add(i, carry):
                    tot = rp[v, f, i].astype(F32) + rq[v, f, i].astype(F32)
                    sp[v, f, i] = tot.astype(BF16)
                    return carry

                lax.fori_loop(0, half, add, 0, unroll=4)
                y2(v, f).start()

        @pl.when(t >= LAG2)
        def _():
            finish(t - LAG2)

        @pl.when(t == 6 + LAG2)
        def _():
            m_wait(mr.at[d_left, rest], m_recv.at[1])
            m_wait(mr.at[d_left, first], m_recv.at[4])
            m_wait(mr.at[d_right], m_recv.at[0])
            m_p1.start()
            m_p2.start()
            m_self.wait()
            for k in range(3):
                m_wait(mr.at[0], m_prel.at[k])
            regroup(xx // 2)

        @pl.when(t == 7 + LAG2)
        def _():
            m_wait(mr.at[d_opp, up], m_recv.at[2])
            m_wait(mr.at[d_opp, lo], m_recv.at[3])
            m_p3.start()
            m_wait(mr.at[0], m_prel.at[3])
            regroup(1 - xx // 2)

        return carry

    lax.fori_loop(0, 8 + LAG2, step, 0)

    for cp in (b_r0, b_r1, b_l1, b_l0, b_fr, b_fl, m_or, m_ol, m_dr, m_dl0, m_dl, m_fr, m_fl, m_p0, m_p1, m_p2, m_p3):
        cp.wait_send()
    for u in (0, 2, 4, 6):
        for p in range(2):
            b_rel(u, p).wait_send()

    def drain(t, carry):
        for f in range(2):
            y1(t, f).wait_send()
            y2(t, f).wait_send()
        return carry

    lax.fori_loop(0, 8, drain, 0)


def solution(mesh):
    n_y, n_d = mesh.shape["seq"], mesh.shape["dap"]
    rep = P()
    in_specs = (P(("data", "seq"), "dap", None), P("data", None), P(("data", "dap"), None, None)) + (rep,) * 8
    out_specs = (P(("data", "dap"), None, None), P(("data", "seq", "dap"), None, None))

    def local_fn(m, mask, z, gamma, beta, w_l, b_l, w_r, b_r, w_o, b_o):
        s_loc, n_i, n_ch = m.shape
        s_all, n_j = mask.shape
        n_e = w_o.shape[1]
        c_hid = w_l.shape[1]
        half = n_i // 2
        hrows = half * c_hid
        s_dev = s_loc // n_d
        vecs = [v.reshape(1, -1) for v in (gamma, beta, b_l, b_r, b_o)]
        any_spec = pl.BlockSpec(memory_space=pl.ANY)
        vm = pl.BlockSpec(memory_space=pltpu.VMEM)
        dma = pltpu.SemaphoreType.DMA
        ysh = (8, 2, half, n_i, n_e)
        z_out, m_out = pl.pallas_call(
            functools.partial(kernel, (n_y, n_d)),
            out_shape=(pltpu.VMEM(z.shape, F32), pltpu.VMEM((s_dev, n_ch, n_j), BF16)),
            in_specs=[any_spec] * 3 + [vm] * 8,
            out_specs=(vm, vm),
            scratch_shapes=[
                pltpu.VMEM((n_i, n_ch, s_loc), BF16),
                pltpu.VMEM((s_all, n_j), jnp.int32),
                pltpu.VMEM((s_loc, n_j), jnp.int32),
                pltpu.VMEM((n_i * n_ch, s_loc), BF16),
                pltpu.VMEM((hrows, half * n_ch), BF16),
                pltpu.VMEM((2, hrows, n_i), BF16),
                pltpu.VMEM((n_i, s_loc), F32),
                pltpu.VMEM((4, s_loc, 256), BF16),
                pltpu.VMEM((8, 2, hrows, s_loc), BF16),
                pltpu.VMEM((c_hid * 128, 4 * n_e), BF16),
                pltpu.VMEM((16, half, c_hid * 128), BF16),
                pltpu.VMEM(ysh, BF16),
                pltpu.VMEM(ysh, BF16),
                pltpu.VMEM(ysh, BF16),
                pltpu.VMEM(ysh, BF16),
                pltpu.VMEM((n_j, 128), F32),
                pltpu.VMEM((n_d, n_i, n_ch, s_loc * 2 // n_d), BF16),
                pltpu.VMEM((2, half, n_ch, s_loc * 2 // n_d), BF16),
                dma((5,)), dma((4,)), dma((2,)), dma((8, 2)), dma((8, 2)),
                dma((3,)), dma((2,)), dma((2,)), dma((4,)), dma((5,)), dma((2,)), dma((4,)),
                dma((8, 2)), dma((8, 2)), dma((8, 2)), dma((8, 2)),
            ],
            compiler_params=pltpu.CompilerParams(collective_id=0, has_side_effects=True, vmem_limit_bytes=VM_LIM * 2**20),
            name="opm",
        )(jnp.transpose(m, (1, 2, 0)), mask, z, *vecs, w_l.T, w_r.T, w_o)
        return z_out, jnp.transpose(m_out, (0, 2, 1))

    return jax.shard_map(local_fn, mesh=mesh, in_specs=in_specs, out_specs=out_specs, check_vma=False)
```

```python
import functools
import jax
import jax.numpy as jnp
from jax import lax
from jax.experimental import pallas as pl
from jax.experimental.pallas import tpu as pltpu
from jax.sharding import PartitionSpec as P

F32 = jnp.float32
BF16 = jnp.bfloat16
LAG1 = 1
LAG2 = 2


def iota(shape, dim):
    return lax.broadcasted_iota(jnp.int32, shape, dim)


def onehot(cond):
    return jnp.where(cond, 1.0, 0.0).astype(BF16)


def dot(a, b):
    return jnp.dot(a, b, preferred_element_type=F32)


def dot_nt(a, b):
    return lax.dot_general(a, b, (((1,), (1,)), ((), ())), preferred_element_type=F32)


def dot_tn(a, b):
    return lax.dot_general(a, b, (((0,), (0,)), ((), ())), preferred_element_type=F32)


def regroup(mr, k, chs, cc):
    _, n_i, _, s_chip = mr.shape
    per = 128 // n_i
    blk = mr[per * k:per * (k + 1), :, chs, :].astype(F32)
    blk = jnp.transpose(blk.reshape(128, blk.shape[2], s_chip), (1, 0, 2))
    blk = jnp.transpose(blk, (0, 2, 1))
    mine = jnp.where(cc == 0, blk[:, 0:s_chip // 2, :], blk[:, s_chip // 2:, :])
    return jnp.transpose(mine, (1, 0, 2)).astype(BF16)


def put_out(z_ref, o_ref, mr, zo_hbm, mo_hbm, last, sem):
    cc = lax.axis_index("dap") % 2
    n_z = z_ref.shape[0] // 4
    n_ch = o_ref.shape[1]
    ch_p = last.shape[1]
    outs = [pltpu.make_async_copy(z_ref.at[k * n_z:(k + 1) * n_z], zo_hbm.at[k * n_z:(k + 1) * n_z], sem.at[k]) for k in range(4)]
    outs.append(pltpu.make_async_copy(o_ref.at[:, 0:n_ch - ch_p], mo_hbm.at[:, 0:n_ch - ch_p], sem.at[4]))
    for o in outs:
        o.start()
    for k in range(last.shape[2] // 128):
        last[:, :, k * 128:(k + 1) * 128] = regroup(mr, k, pl.ds(n_ch - ch_p, ch_p), cc)
    tail = pltpu.make_async_copy(last, mo_hbm.at[:, n_ch - ch_p:], sem.at[5])
    tail.start()
    for o in outs + [tail]:
        o.wait()


def kernel(dims, m_hbm, mask_hbm, z_hbm, *refs):
    smalls_hbm, refs = refs[:8], refs[8:]
    (zv, ov, mr), refs = refs[:3], refs[3:]
    smalls, refs = refs[:8], refs[8:]
    gam, bet, bias_l, bias_r, bias_o, waT, wbT, wo = smalls
    (mT, mkv, mkl, xT, wbig, bbb, mkT, acat, bT, wblk, lbuf, rp, rq, sp, sq, rc, tbuf,
     sem_in, sem_small, bs_own, bs_fwd, bs_rel, b_recv, ms_dir, ms_opp, ms_fwd, ms_rel, m_recv, mo_recv, mf_recv, m_prel,
           y1s, y1r, y2s, y2r) = refs
    n_y, n_d = dims
    n_x = n_d // 2
    yy = lax.axis_index("seq")
    dd = lax.axis_index("dap")
    xx = dd // 2
    cc = dd % 2
    x_r = (xx + 1) % n_x
    x_l = (xx + n_x - 1) % n_x
    x_o = (xx + 2) % n_x
    right, left, mate = 2 * x_r + cc, 2 * x_l + cc, 2 * xx + 1 - cc
    par = yy % 2
    y_a = yy + 1 - 2 * par
    y_b = (yy + n_y - 1 + 2 * par) % n_y
    n_i, n_ch, s_loc = mT.shape
    s_all, n_j = mkv.shape
    c_hid = waT.shape[0]
    half = n_i // 2
    hrows = half * c_hid
    s_chip = s_loc // n_x
    s_dev = s_loc // n_d

    def to_dap(idx):
        return dict(device_id={"dap": idx}, device_id_type=pl.DeviceIdType.MESH)

    def to_seq(idx):
        return dict(device_id={"seq": idx}, device_id_type=pl.DeviceIdType.MESH)

    in_m = pltpu.make_async_copy(m_hbm, mT, sem_in.at[0])
    mine_rows = pl.ds(pl.multiple_of(yy * s_loc, s_loc), s_loc)
    in_mloc = pltpu.make_async_copy(mask_hbm.at[mine_rows], mkl, sem_in.at[4])
    in_mask = pltpu.make_async_copy(mask_hbm, mkv, sem_in.at[1])
    in_z = pltpu.make_async_copy(z_hbm, zv, sem_in.at[2])

    in_small = [pltpu.make_async_copy(a, b, sem_small.at[k]) for k, (a, b) in enumerate(zip(smalls_hbm, smalls))]

    barrier = pltpu.get_barrier_semaphore()
    for nb in (right, left, mate):
        pl.semaphore_signal(barrier, inc=1, **to_dap(nb))
    for nb in (y_a, y_b):
        pl.semaphore_signal(barrier, inc=1, **to_seq(nb))

    in_m.start()
    in_mloc.start()
    for cp in in_small:
        cp.start()

    def remote(src, dst, ssem, rsem, to):
        return pltpu.make_async_remote_copy(src_ref=src, dst_ref=dst, send_sem=ssem, recv_sem=rsem, **to)

    def b_to(src_u, src_p, dst_u, dst_p, ssem, nb):
        return remote(bT.at[src_u, src_p], bT.at[dst_u, dst_p], ssem, b_recv.at[dst_u, dst_p], to_dap(nb))

    b_r0 = b_to(0, 0, 2, 0, bs_own.at[0], right)
    b_r1 = b_to(0, 1, 4, 0, bs_own.at[1], right)
    b_l1 = b_to(0, 1, 2, 1, bs_own.at[2], left)
    b_l0 = b_to(0, 0, 4, 1, bs_own.at[3], left)
    b_fr = b_to(2, 0, 6, 0, bs_fwd.at[0], right)
    b_fl = b_to(2, 1, 6, 1, bs_fwd.at[1], left)

    def b_rel(u, p):
        return b_to(u, p, u + 1, p, bs_rel.at[u, p], mate)

    def b_wait(u, p):
        b_to(u, p, u, p, bs_rel.at[u, p], mate).wait_recv()

    def lanes_of(xc):
        return pl.ds(pl.multiple_of(xc * s_chip, s_chip), s_chip)

    d_right, d_left, d_opp = 2 * x_r + cc, 2 * x_l + cc, 2 * x_o + cc
    up, lo = pl.ds(0, half), pl.ds(half, half)
    m_or = remote(m_hbm.at[up, :, lanes_of(x_o)], tbuf.at[0], ms_opp.at[0], mf_recv.at[0], to_dap(right))
    m_ol = remote(m_hbm.at[lo, :, lanes_of(x_o)], tbuf.at[1], ms_opp.at[1], mf_recv.at[1], to_dap(left))
    n_p = 4
    ch_p = n_ch // n_p

    def m_dir(k, p):
        chs = pl.ds(pl.multiple_of(p * ch_p, ch_p), ch_p)
        src = m_hbm.at[:, chs, lanes_of(x_l if k else x_r)]
        return remote(src, mr.at[dd, :, chs], ms_dir.at[k, p], m_recv.at[k, p], to_dap(left if k else right))

    def m_rel(k, p):
        chs = pl.ds(pl.multiple_of(p * ch_p, ch_p), ch_p)
        ref = mr.at[d_right if k == 0 else d_left, :, chs]
        return remote(ref, ref, ms_rel.at[k, p], m_prel.at[k, p], to_dap(mate))

    m_fr = remote(tbuf.at[0], mr.at[d_left, up], ms_fwd.at[0], mo_recv.at[0], to_dap(right))
    m_fl = remote(tbuf.at[1], mr.at[d_right, lo], ms_fwd.at[1], mo_recv.at[1], to_dap(left))
    m_p0 = remote(m_hbm.at[:, :, lanes_of(xx)], mr.at[dd], ms_rel.at[2, 0], m_prel.at[2, 0], to_dap(mate))
    m_p3 = [remote(mr.at[d_opp, rows], mr.at[d_opp, rows], ms_rel.at[2, 1 + k], m_prel.at[2, 1 + k], to_dap(mate))
            for k, rows in enumerate((up, lo))]
    m_self = pltpu.make_async_copy(m_hbm.at[:, :, lanes_of(xx)], mr.at[dd], sem_in.at[3])

    pl.semaphore_wait(barrier, 5)
    m_or.start()
    m_ol.start()
    m_p0.start()

    for cp in in_small:
        cp.wait()
    def column(row, n, wide):
        eye = iota((n, n), 0) == iota((n, n), 1)
        diag = jnp.where(eye, jnp.broadcast_to(row, (n, n)), 0.0).astype(BF16)
        return dot(diag, jnp.ones((n, wide), BF16))

    lw = s_loc // 2
    gcol = column(gam[...].astype(F32), n_ch, lw)
    bcol = column(bet[...].astype(F32), n_ch, lw)
    blc = column(bias_l[...].astype(F32), c_hid, 128)
    brc = column(bias_r[...].astype(F32), c_hid, 128)
    kb = half * n_ch
    wide = dot(wbT[...], onehot((iota((n_ch, kb), 1) & (n_ch - 1)) == iota((n_ch, kb), 0)))
    keep = iota((half, kb), 0) == iota((half, kb), 1) // n_ch
    lane_i = iota((half, n_i), 1) - iota((half, n_i), 0)
    for d in range(c_hid):
        rows = slice(d * half, (d + 1) * half)
        wbig[rows, :] = jnp.where(keep, jnp.broadcast_to(wide[d:d + 1, :], (half, kb)), 0.0).astype(BF16)
        bias = jnp.broadcast_to(brc[d:d + 1, 0:n_i], (half, n_i))
        for h in range(2):
            bbb[h, rows, :] = jnp.where(lane_i == h * half, bias, 0.0).astype(BF16)

    in_mloc.wait()
    selT = onehot(iota((n_i, n_j), 1) == iota((n_i, n_j), 0) + dd * n_i)
    mkT[...] = dot_nt(selT, mkl[...].astype(F32).astype(BF16))
    in_m.wait()

    ga = 128 // c_hid
    n_e = wo.shape[1]
    pos = iota((128, c_hid * c_hid), 0)
    want = (pos & (c_hid - 1)) * c_hid + pos // c_hid
    gap = iota((128, c_hid * c_hid), 1) - want

    def place(dc, carry):
        wp = dot(onehot(gap == dc * ga), wo[...]).astype(BF16)
        for k in range(ga):
            for i4 in range(ga):
                row = pl.multiple_of((dc * ga + k) * 128 + i4 * c_hid, c_hid)
                wblk[pl.ds(row, c_hid), i4 * n_e:(i4 + 1) * n_e] = wp[k * c_hid:(k + 1) * c_hid, :]
        return carry

    def norm_row(r, carry):
        for q in range(2):
            lanes = slice(q * lw, (q + 1) * lw)
            act = mT[r, :, lanes].astype(F32)
            mean = jnp.sum(act, axis=0, keepdims=True) * (1.0 / n_ch)
            cen = act - mean
            var = jnp.sum(cen * cen, axis=0, keepdims=True) * (1.0 / n_ch)
            nrm = cen * lax.rsqrt(var + 1e-5)
            val = (nrm * gcol + bcol).astype(BF16) * mkT[pl.ds(r, 1), lanes].astype(BF16)
            xT[pl.ds(pl.multiple_of(r * n_ch, n_ch), n_ch), lanes] = val
        return carry

    mk16 = mkT[...].astype(BF16)
    for h in range(2):
        lax.fori_loop(h * half, (h + 1) * half, norm_row, 0, unroll=2)
        acc = dot(wbig[...], xT[h * kb:(h + 1) * kb, :]) + dot(bbb[h], mk16)
        bT[0, h] = acc.astype(BF16)
        if h == 0:
            b_r0.start()
        else:
            b_l1.start()
            b_l0.start()
            b_r1.start()
        b_rel(0, h).start()
    m_self.start()
    in_mask.start()
    in_z.start()

    ka = ga * n_ch
    ra = onehot((iota((128, c_hid), 0) & (c_hid - 1)) == iota((128, c_hid), 1))
    wa_rep = dot(dot(ra, waT[...]).astype(BF16), onehot((iota((n_ch, ka), 1) & (n_ch - 1)) == iota((n_ch, ka), 0)))
    wa4 = jnp.where(iota((128, ka), 0) // c_hid == iota((128, ka), 1) // n_ch, wa_rep, 0.0).astype(BF16)
    ba_rep = dot(ra, blc.astype(BF16))[:, 0:n_i]
    lane_a = iota((128, n_i), 1) - iota((128, n_i), 0) // c_hid
    n_g = n_i // ga
    for g in range(n_g):
        bag = jnp.where(lane_a == ga * g, ba_rep, 0.0).astype(BF16)
        at = dot(wa4, xT[g * ka:(g + 1) * ka, :]) + dot(bag, mk16)
        acat[g // 2, :, (g % 2) * 128:(g % 2 + 1) * 128] = at.T.astype(BF16)

    wblk[...] = jnp.zeros_like(wblk)
    lax.fori_loop(0, c_hid // ga, place, 0, unroll=4)

    def pair_counts():
        sel = onehot(iota((n_j, 128), 0) == iota((n_j, 128), 1) + dd * n_i)
        rc[...] = jnp.zeros_like(rc)

        def add(k, carry):
            mk = mkv[pl.ds(pl.multiple_of(k * s_loc, s_loc), s_loc), :].astype(F32).astype(BF16)
            rc[...] += dot_tn(mk, dot(mk, sel).astype(BF16))
            return carry

        lax.fori_loop(0, s_all // s_loc, add, 0, unroll=2)
        rc[...] = 1.0 / (1e-3 + rc[...])

    def compute(t):
        lhs = bT[t].reshape(2 * hrows, s_loc)
        for n in range(4):
            acc = dot(lhs, acat[n]).astype(BF16)
            for h in range(2):
                for d in range(c_hid):
                    row = (h * c_hid + d) * half
                    for gg in range(2):
                        lbuf[(2 * n + gg) * 2 + h, :, d * 128:(d + 1) * 128] = acc[row:row + half, gg * 128:(gg + 1) * 128]
        for nn in range(2):
            cols = slice(nn * 256, (nn + 1) * 256)
            res = dot(lbuf[...].reshape(n_g * n_i, c_hid * 128), wblk[:, cols]).astype(BF16)
            for g in range(n_g):
                for k in range(2):
                    i = ga * g + 2 * nn + k
                    rp[t, i // half, i % half] = res[g * n_i:(g + 1) * n_i, k * 128:(k + 1) * 128]

    def y1(t, f):
        return remote(rp.at[t, f], rq.at[t, f], y1s.at[t, f], y1r.at[t, f], to_seq(y_a if f == 0 else y_b))

    def y2(t, f):
        return remote(sp.at[t, f], sq.at[t, f], y2s.at[t, f], y2r.at[t, f], to_seq(y_b if f == 0 else y_a))

    def j_of(t, p):
        u = t // 2
        off = jnp.where(u == 0, 0, jnp.where(u == 3, 2, n_x - 1 if p == 0 else 1))
        core = jnp.where(t % 2 == 0, cc, 1 - cc)
        hh = jnp.where(u == 2, 1 - p, p)
        return pl.multiple_of((2 * ((xx + off) % n_x) + core) * n_i + hh * half, half)

    def finish(t):
        bo = bias_o[...].astype(F32)
        for f in range(2):
            y2(t, f).wait_recv()
        for p in range(2):
            j0 = j_of(t, p)
            rcp = rc[pl.ds(j0, half), :]
            for i in range(n_i):
                rows = slice(p * half, (p + 1) * half)
                tot = sp[t, i // half, i % half, rows, :].astype(F32) + sq[t, i // half, i % half, rows, :].astype(F32)
                upd = (tot + bo) * jnp.broadcast_to(rcp[:, i:i + 1], (half, n_e))
                zv[i, pl.ds(j0, half), :] += upd

    per = 128 // n_i

    def m_land(p):
        for k in range(2):
            m_dir(k, p).wait_recv()
            m_rel(1 - k, p).start()

    def m_part(p):
        for k in range(2):
            m_rel(k, p).wait_recv()
        if p < n_p - 1:
            chs = pl.ds(p * ch_p, ch_p)
            for k in range(n_d // per):
                ov[:, chs, k * 128:(k + 1) * 128] = regroup(mr, k, chs, cc)

    def step(t, carry):
        @pl.when(t == 1)
        def _():
            b_wait(1, 0)
            b_wait(1, 1)

        @pl.when(t == 2)
        def _():
            in_mask.wait()
            in_z.wait()
            pair_counts()
            b_wait(2, 0)
            b_fr.start()
            b_rel(2, 0).start()
            b_wait(2, 1)
            b_fl.start()
            b_rel(2, 1).start()
            m_or.wait_recv()
            m_fr.start()
            m_ol.wait_recv()
            m_fl.start()
            for p in range(n_p):
                m_dir(0, p).start()
                m_dir(1, p).start()

        @pl.when(t == 3)
        def _():
            b_wait(3, 0)
            b_wait(3, 1)

        @pl.when(t == 4)
        def _():
            b_wait(4, 0)
            b_rel(4, 0).start()
            b_wait(4, 1)
            b_rel(4, 1).start()

        @pl.when(t == 5)
        def _():
            b_wait(5, 0)
            b_wait(5, 1)

        @pl.when(t == 6)
        def _():
            b_wait(6, 0)
            b_rel(6, 0).start()
            b_wait(6, 1)
            b_rel(6, 1).start()

        @pl.when(t == 7)
        def _():
            b_wait(7, 0)
            b_wait(7, 1)

        @pl.when(t < 8)
        def _():
            compute(t)
            for f in range(2):
                y1(t, f).start()

        @pl.when(jnp.logical_and(t >= LAG1, t < 8 + LAG1))
        def _():
            v = t - LAG1
            for f in range(2):
                y1(v, f).wait_recv()

                def add(i, carry):
                    tot = rp[v, f, i].astype(F32) + rq[v, f, i].astype(F32)
                    sp[v, f, i] = tot.astype(BF16)
                    return carry

                lax.fori_loop(0, half, add, 0, unroll=4)
                y2(v, f).start()

        @pl.when(t == 6 + LAG2)
        def _():
            m_self.wait()
            for k in range(2):
                m_fr.wait_recv() if k == 0 else m_fl.wait_recv()
                m_p3[k].start()
            m_land(0)
            m_p0.wait_recv()
            for k in range(2):
                m_p3[k].wait_recv()
            m_land(1)
            m_part(0)

        @pl.when(t >= LAG2)
        def _():
            finish(t - LAG2)

        @pl.when(t == 7 + LAG2)
        def _():
            for p in range(2, n_p):
                m_land(p)
                m_part(p - 1)
            m_part(n_p - 1)

        return carry

    lax.fori_loop(0, 8 + LAG2, step, 0)

    for cp in (b_r0, b_r1, b_l1, b_l0, b_fr, b_fl, m_or, m_ol, m_fr, m_fl, m_p0, *m_p3):
        cp.wait_send()
    for k in range(2):
        for p in range(n_p):
            m_dir(k, p).wait_send()
            m_rel(k, p).wait_send()
    for u in (0, 2, 4, 6):
        for p in range(2):
            b_rel(u, p).wait_send()

    def drain(t, carry):
        for f in range(2):
            y1(t, f).wait_send()
            y2(t, f).wait_send()
        return carry

    lax.fori_loop(0, 8, drain, 0)


def solution(mesh):
    n_y, n_d = mesh.shape["seq"], mesh.shape["dap"]
    rep = P()
    in_specs = (P(("data", "seq"), "dap", None), P("data", None), P(("data", "dap"), None, None)) + (rep,) * 8
    out_specs = (P(("data", "dap"), None, None), P(("data", "seq", "dap"), None, None))

    def local_fn(m, mask, z, gamma, beta, w_l, b_l, w_r, b_r, w_o, b_o):
        s_loc, n_i, n_ch = m.shape
        s_all, n_j = mask.shape
        n_e = w_o.shape[1]
        c_hid = w_l.shape[1]
        half = n_i // 2
        hrows = half * c_hid
        s_dev = s_loc // n_d
        vecs = [v.reshape(1, -1) for v in (gamma, beta, b_l, b_r, b_o)]
        smalls = (*vecs, w_l.T, w_r.T, w_o)
        any_spec = pl.BlockSpec(memory_space=pl.ANY)
        vm = pl.BlockSpec(memory_space=pltpu.VMEM)
        dma = pltpu.SemaphoreType.DMA
        ysh = (8, 2, half, n_i, n_e)
        mr_shape = (n_d, n_i, n_ch, s_loc * 2 // n_d)
        held = pl.pallas_call(
            functools.partial(kernel, (n_y, n_d)),
            out_shape=(pltpu.VMEM(z.shape, F32), pltpu.VMEM((s_dev, n_ch, n_j), BF16), pltpu.VMEM(mr_shape, BF16)),
            in_specs=[any_spec] * 11,
            out_specs=(vm, vm, vm),
            scratch_shapes=[pltpu.VMEM(v.shape, BF16) for v in smalls] + [
                pltpu.VMEM((n_i, n_ch, s_loc), BF16),
                pltpu.VMEM((s_all, n_j), jnp.int32),
                pltpu.VMEM((s_loc, n_j), jnp.int32),
                pltpu.VMEM((n_i * n_ch, s_loc), BF16),
                pltpu.VMEM((hrows, half * n_ch), BF16),
                pltpu.VMEM((2, hrows, n_i), BF16),
                pltpu.VMEM((n_i, s_loc), F32),
                pltpu.VMEM((4, s_loc, 256), BF16),
                pltpu.VMEM((8, 2, hrows, s_loc), BF16),
                pltpu.VMEM((c_hid * 128, 4 * n_e), BF16),
                pltpu.VMEM((16, half, c_hid * 128), BF16),
                pltpu.VMEM(ysh, BF16),
                pltpu.VMEM(ysh, BF16),
                pltpu.VMEM(ysh, BF16),
                pltpu.VMEM(ysh, BF16),
                pltpu.VMEM((n_j, 128), F32),
                pltpu.VMEM((2, half, n_ch, s_loc * 2 // n_d), BF16),
                dma((5,)), dma((8,)), dma((4,)), dma((2,)), dma((8, 2)), dma((8, 2)),
                dma((2, 4)), dma((2,)), dma((2,)), dma((3, 4)), dma((2, 4)), dma((2,)), dma((2,)), dma((3, 4)),
                dma((8, 2)), dma((8, 2)), dma((8, 2)), dma((8, 2)),
            ],
            compiler_params=pltpu.CompilerParams(collective_id=0, has_side_effects=True, vmem_limit_bytes=52 * 2**20),
            name="opm",
        )(jnp.transpose(m, (1, 2, 0)), mask, z, *smalls)
        z_out, m_out = pl.pallas_call(
            put_out,
            out_shape=(jax.ShapeDtypeStruct(z.shape, F32), jax.ShapeDtypeStruct((s_dev, n_ch, n_j), BF16)),
            in_specs=[vm] * 3,
            out_specs=(any_spec, any_spec),
            scratch_shapes=[pltpu.VMEM((s_dev, n_ch // 4, n_j), BF16), dma((6,))],
            compiler_params=pltpu.CompilerParams(vmem_limit_bytes=10 * 2**20),
            name="out",
        )(*held)
        return z_out, jnp.transpose(m_out, (0, 2, 1))

    return jax.shard_map(local_fn, mesh=mesh, in_specs=in_specs, out_specs=out_specs, check_vma=False)
```

```python
import functools
import jax
import jax.numpy as jnp
from jax import lax
from jax.experimental import pallas as pl
from jax.experimental.pallas import tpu as pltpu
from jax.sharding import PartitionSpec as P

F32 = jnp.float32
BF16 = jnp.bfloat16
LAG1 = 1
LAG2 = 3


def iota(shape, dim):
    return lax.broadcasted_iota(jnp.int32, shape, dim)


def onehot(cond):
    return jnp.where(cond, 1.0, 0.0).astype(BF16)


def dot(a, b):
    return jnp.dot(a, b, preferred_element_type=F32)


def dot_nt(a, b):
    return lax.dot_general(a, b, (((1,), (1,)), ((), ())), preferred_element_type=F32)


def dot_tn(a, b):
    return lax.dot_general(a, b, (((0,), (0,)), ((), ())), preferred_element_type=F32)


def regroup(mr, k, chs, cc):
    _, n_i, _, s_chip = mr.shape
    per = 128 // n_i
    blk = mr[per * k:per * (k + 1), :, chs, :].astype(F32)
    blk = jnp.transpose(blk.reshape(128, blk.shape[2], s_chip), (1, 0, 2))
    blk = jnp.transpose(blk, (0, 2, 1))
    mine = jnp.where(cc == 0, blk[:, 0:s_chip // 2, :], blk[:, s_chip // 2:, :])
    return jnp.transpose(mine, (1, 0, 2)).astype(BF16)


def put_out(z_ref, o_ref, mr, zo_hbm, mo_hbm, last, sem):
    cc = lax.axis_index("dap") % 2
    n_z = z_ref.shape[0] // 4
    n_ch = o_ref.shape[1]
    ch_p = last.shape[1]
    outs = [pltpu.make_async_copy(z_ref.at[k * n_z:(k + 1) * n_z], zo_hbm.at[k * n_z:(k + 1) * n_z], sem.at[k]) for k in range(4)]
    outs.append(pltpu.make_async_copy(o_ref.at[:, 0:n_ch - ch_p], mo_hbm.at[:, 0:n_ch - ch_p], sem.at[4]))
    for o in outs:
        o.start()
    for k in range(last.shape[2] // 128):
        last[:, :, k * 128:(k + 1) * 128] = regroup(mr, k, pl.ds(n_ch - ch_p, ch_p), cc)
    tail = pltpu.make_async_copy(last, mo_hbm.at[:, n_ch - ch_p:], sem.at[5])
    tail.start()
    for o in outs + [tail]:
        o.wait()


def kernel(dims, m_hbm, mask_hbm, z_hbm, *refs):
    smalls_hbm, refs = refs[:8], refs[8:]
    (zv, ov, mr), refs = refs[:3], refs[3:]
    smalls, refs = refs[:8], refs[8:]
    gam, bet, bias_l, bias_r, bias_o, waT, wbT, wo = smalls
    (mT, mkv, mkl, xT, wbig, bbb, mkT, acat, bT, wblk, lbuf, rp, rq, sp, sq, rc, tbuf, gb, mko,
     sem_in, sem_small, bs_own, bs_fwd, bs_rel, b_recv, bs_cut, bc_recv, ms_dir, ms_opp, ms_fwd, ms_rel, m_recv, mo_recv, mf_recv, m_prel,
           y1s, y1r, y2s, y2r) = refs
    n_y, n_d = dims
    n_x = n_d // 2
    yy = lax.axis_index("seq")
    dd = lax.axis_index("dap")
    xx = dd // 2
    cc = dd % 2
    x_r = (xx + 1) % n_x
    x_l = (xx + n_x - 1) % n_x
    x_o = (xx + 2) % n_x
    right, left, mate = 2 * x_r + cc, 2 * x_l + cc, 2 * xx + 1 - cc
    par = yy % 2
    y_a = yy + 1 - 2 * par
    y_b = (yy + n_y - 1 + 2 * par) % n_y
    n_i, n_ch, s_loc = mT.shape
    s_all, n_j = mkv.shape
    c_hid = waT.shape[0]
    half = n_i // 2
    hrows = half * c_hid
    s_chip = s_loc // n_x
    s_dev = s_loc // n_d

    def to_dap(idx):
        return dict(device_id={"dap": idx}, device_id_type=pl.DeviceIdType.MESH)

    def to_seq(idx):
        return dict(device_id={"seq": idx}, device_id_type=pl.DeviceIdType.MESH)

    in_m = pltpu.make_async_copy(m_hbm, mT, sem_in.at[0])
    mine_rows = pl.ds(pl.multiple_of(yy * s_loc, s_loc), s_loc)
    in_mloc = pltpu.make_async_copy(mask_hbm.at[mine_rows], mkl, sem_in.at[4])
    in_mask = pltpu.make_async_copy(mask_hbm, mkv, sem_in.at[1])
    in_z = pltpu.make_async_copy(z_hbm, zv, sem_in.at[2])

    in_small = [pltpu.make_async_copy(a, b, sem_small.at[k]) for k, (a, b) in enumerate(zip(smalls_hbm, smalls))]

    barrier = pltpu.get_barrier_semaphore()
    for nb in (right, left, mate):
        pl.semaphore_signal(barrier, inc=1, **to_dap(nb))
    for nb in (y_a, y_b):
        pl.semaphore_signal(barrier, inc=1, **to_seq(nb))

    in_m.start()
    in_mloc.start()
    for cp in in_small:
        cp.start()

    def remote(src, dst, ssem, rsem, to):
        return pltpu.make_async_remote_copy(src_ref=src, dst_ref=dst, send_sem=ssem, recv_sem=rsem, **to)

    def lanes_of(xc):
        return pl.ds(pl.multiple_of(xc * s_chip, s_chip), s_chip)

    def b_to(src_u, src_p, dst_u, dst_p, ssem, nb):
        return remote(bT.at[src_u, src_p], bT.at[dst_u, dst_p], ssem, b_recv.at[dst_u, dst_p], to_dap(nb))

    n_f = n_x - 1

    def b_cut(p, k):
        cols = lanes_of((x_o + 1 + k) % n_x)
        src, dst = bT.at[0, p, :, cols], bT.at[2, p, :, cols]
        return remote(src, dst, bs_cut.at[p, k], bc_recv.at[p, k], to_dap(left if p else right))

    b_r1 = b_to(0, 1, 4, 0, bs_own.at[1], right)
    b_l0 = b_to(0, 0, 4, 1, bs_own.at[3], left)
    b_fr = b_to(2, 0, 6, 0, bs_fwd.at[0], right)
    b_fl = b_to(2, 1, 6, 1, bs_fwd.at[1], left)

    def b_rel(u, p):
        return b_to(u, p, u + 1, p, bs_rel.at[u, p], mate)

    def b_wait(u, p):
        b_to(u, p, u, p, bs_rel.at[u, p], mate).wait_recv()

    d_right, d_left, d_opp = 2 * x_r + cc, 2 * x_l + cc, 2 * x_o + cc
    up, lo = pl.ds(0, half), pl.ds(half, half)
    m_or = remote(m_hbm.at[up, :, lanes_of(x_o)], tbuf.at[0], ms_opp.at[0], mf_recv.at[0], to_dap(right))
    m_ol = remote(m_hbm.at[lo, :, lanes_of(x_o)], tbuf.at[1], ms_opp.at[1], mf_recv.at[1], to_dap(left))
    n_p = 4
    ch_p = n_ch // n_p

    def m_dir(k, p):
        chs = pl.ds(pl.multiple_of(p * ch_p, ch_p), ch_p)
        src = m_hbm.at[:, chs, lanes_of(x_l if k else x_r)]
        return remote(src, mr.at[dd, :, chs], ms_dir.at[k, p], m_recv.at[k, p], to_dap(left if k else right))

    def m_rel(k, p):
        chs = pl.ds(pl.multiple_of(p * ch_p, ch_p), ch_p)
        ref = mr.at[d_right if k == 0 else d_left, :, chs]
        return remote(ref, ref, ms_rel.at[k, p], m_prel.at[k, p], to_dap(mate))

    m_fr = remote(tbuf.at[0], mr.at[d_left, up], ms_fwd.at[0], mo_recv.at[0], to_dap(right))
    m_fl = remote(tbuf.at[1], mr.at[d_right, lo], ms_fwd.at[1], mo_recv.at[1], to_dap(left))
    m_p0 = remote(m_hbm.at[:, :, lanes_of(xx)], mr.at[dd], ms_rel.at[2, 0], m_prel.at[2, 0], to_dap(mate))
    m_p3 = [remote(mr.at[d_opp, rows], mr.at[d_opp, rows], ms_rel.at[2, 1 + k], m_prel.at[2, 1 + k], to_dap(mate))
            for k, rows in enumerate((up, lo))]
    m_self = pltpu.make_async_copy(m_hbm.at[:, :, lanes_of(xx)], mr.at[dd], sem_in.at[3])

    pl.semaphore_wait(barrier, 5)
    m_or.start()
    m_ol.start()
    m_p0.start()

    wblk[...] = jnp.zeros_like(wblk)

    for cp in in_small:
        cp.wait()
    def column(row, n, wide):
        eye = iota((n, n), 0) == iota((n, n), 1)
        diag = jnp.where(eye, jnp.broadcast_to(row, (n, n)), 0.0).astype(BF16)
        return dot(diag, jnp.ones((n, wide), BF16))

    lw = s_loc // 2
    gcol = column(gam[...].astype(F32), n_ch, lw)
    bcol = column(bet[...].astype(F32), n_ch, lw)
    gb[0] = gcol[:, 0:s_chip]
    gb[1] = bcol[:, 0:s_chip]
    blc = column(bias_l[...].astype(F32), c_hid, 128)
    brc = column(bias_r[...].astype(F32), c_hid, 128)
    kb = half * n_ch
    wide = dot(wbT[...], onehot((iota((n_ch, kb), 1) & (n_ch - 1)) == iota((n_ch, kb), 0)))
    keep = iota((half, kb), 0) == iota((half, kb), 1) // n_ch
    lane_i = iota((half, n_i), 1) - iota((half, n_i), 0)
    for d in range(c_hid):
        rows = slice(d * half, (d + 1) * half)
        wbig[rows, :] = jnp.where(keep, jnp.broadcast_to(wide[d:d + 1, :], (half, kb)), 0.0).astype(BF16)
        bias = jnp.broadcast_to(brc[d:d + 1, 0:n_i], (half, n_i))
        for h in range(2):
            bbb[h, rows, :] = jnp.where(lane_i == h * half, bias, 0.0).astype(BF16)

    in_mloc.wait()
    selT = onehot(iota((n_i, n_j), 1) == iota((n_i, n_j), 0) + dd * n_i)
    mkT[...] = dot_nt(selT, mkl[...].astype(F32).astype(BF16))
    in_m.wait()

    ga = 128 // c_hid
    n_e = wo.shape[1]
    pos = iota((128, c_hid * c_hid), 0)
    want = (pos & (c_hid - 1)) * c_hid + pos // c_hid
    gap = iota((128, c_hid * c_hid), 1) - want

    def place(dc, carry):
        wp = dot(onehot(gap == dc * ga), wo[...]).astype(BF16)
        for k in range(ga):
            for i4 in range(ga):
                row = pl.multiple_of((dc * ga + k) * 128 + i4 * c_hid, c_hid)
                wblk[pl.ds(row, c_hid), i4 * n_e:(i4 + 1) * n_e] = wp[k * c_hid:(k + 1) * c_hid, :]
        return carry

    def norm_row(r, carry):
        for q in range(2):
            lanes = slice(q * lw, (q + 1) * lw)
            act = mT[r, :, lanes].astype(F32)
            mean = jnp.sum(act, axis=0, keepdims=True) * (1.0 / n_ch)
            cen = act - mean
            var = jnp.sum(cen * cen, axis=0, keepdims=True) * (1.0 / n_ch)
            nrm = cen * lax.rsqrt(var + 1e-5)
            val = (nrm * gcol + bcol).astype(BF16) * mkT[pl.ds(r, 1), lanes].astype(BF16)
            xT[pl.ds(pl.multiple_of(r * n_ch, n_ch), n_ch), lanes] = val
        return carry

    mk16 = mkT[...].astype(BF16)
    for h in range(2):
        lax.fori_loop(h * half, (h + 1) * half, norm_row, 0, unroll=2)
        acc = dot(wbig[...], xT[h * kb:(h + 1) * kb, :]) + dot(bbb[h], mk16)
        bT[0, h] = acc.astype(BF16)
        if h == 0:
            for k in range(n_f):
                b_cut(0, k).start()
        else:
            for k in range(n_f):
                b_cut(1, k).start()
            b_l0.start()
            b_r1.start()
        b_rel(0, h).start()
    m_self.start()
    in_mask.start()
    in_z.start()

    ka = ga * n_ch
    ra = onehot((iota((128, c_hid), 0) & (c_hid - 1)) == iota((128, c_hid), 1))
    wa_rep = dot(dot(ra, waT[...]).astype(BF16), onehot((iota((n_ch, ka), 1) & (n_ch - 1)) == iota((n_ch, ka), 0)))
    wa4 = jnp.where(iota((128, ka), 0) // c_hid == iota((128, ka), 1) // n_ch, wa_rep, 0.0).astype(BF16)
    ba_rep = dot(ra, blc.astype(BF16))[:, 0:n_i]
    lane_a = iota((128, n_i), 1) - iota((128, n_i), 0) // c_hid
    n_g = n_i // ga
    for g in range(n_g):
        bag = jnp.where(lane_a == ga * g, ba_rep, 0.0).astype(BF16)
        at = dot(wa4, xT[g * ka:(g + 1) * ka, :]) + dot(bag, mk16)
        acat[g // 2, :, (g % 2) * 128:(g % 2 + 1) * 128] = at.T.astype(BF16)

    lax.fori_loop(0, c_hid // ga, place, 0, unroll=4)

    def pair_counts():
        sel = onehot(iota((n_j, 128), 0) == iota((n_j, 128), 1) + dd * n_i)
        rc[...] = jnp.zeros_like(rc)

        def add(k, carry):
            mk = mkv[pl.ds(pl.multiple_of(k * s_loc, s_loc), s_loc), :].astype(F32).astype(BF16)
            rc[...] += dot_tn(mk, dot(mk, sel).astype(BF16))
            return carry

        lax.fori_loop(0, s_all // s_loc, add, 0, unroll=2)
        rc[...] = 1.0 / (1e-3 + rc[...])

    def compute(t):
        lhs = bT[t].reshape(2 * hrows, s_loc)
        for n in range(4):
            acc = dot(lhs, acat[n]).astype(BF16)
            for h in range(2):
                for d in range(c_hid):
                    row = (h * c_hid + d) * half
                    for gg in range(2):
                        lbuf[(2 * n + gg) * 2 + h, :, d * 128:(d + 1) * 128] = acc[row:row + half, gg * 128:(gg + 1) * 128]
        for nn in range(2):
            cols = slice(nn * 256, (nn + 1) * 256)
            res = dot(lbuf[...].reshape(n_g * n_i, c_hid * 128), wblk[:, cols]).astype(BF16)
            for g in range(n_g):
                for k in range(2):
                    i = ga * g + 2 * nn + k
                    rp[t, i // half, i % half] = res[g * n_i:(g + 1) * n_i, k * 128:(k + 1) * 128]

    def y1(t, f):
        return remote(rp.at[t, f], rq.at[t, f], y1s.at[t, f], y1r.at[t, f], to_seq(y_a if f == 0 else y_b))

    def y2(t, f):
        return remote(sp.at[t, f], sq.at[t, f], y2s.at[t, f], y2r.at[t, f], to_seq(y_b if f == 0 else y_a))

    def j_of(t, p):
        u = t // 2
        off = jnp.where(u == 0, 0, jnp.where(u == 3, 2, n_x - 1 if p == 0 else 1))
        core = jnp.where(t % 2 == 0, cc, 1 - cc)
        hh = jnp.where(u == 2, 1 - p, p)
        return pl.multiple_of((2 * ((xx + off) % n_x) + core) * n_i + hh * half, half)

    def finish(t):
        bo = bias_o[...].astype(F32)
        for f in range(2):
            y2(t, f).wait_recv()
        for p in range(2):
            j0 = j_of(t, p)
            rcp = rc[pl.ds(j0, half), :]
            for i in range(n_i):
                rows = slice(p * half, (p + 1) * half)
                tot = sp[t, i // half, i % half, rows, :].astype(F32) + sq[t, i // half, i % half, rows, :].astype(F32)
                upd = (tot + bo) * jnp.broadcast_to(rcp[:, i:i + 1], (half, n_e))
                zv[i, pl.ds(j0, half), :] += upd

    per = 128 // n_i

    def m_land(p):
        for k in range(2):
            m_dir(k, p).wait_recv()
            m_rel(1 - k, p).start()

    def m_part(p):
        for k in range(2):
            m_rel(k, p).wait_recv()
        if p < n_p - 1:
            chs = pl.ds(p * ch_p, ch_p)
            for k in range(n_d // per):
                ov[:, chs, k * 128:(k + 1) * 128] = regroup(mr, k, chs, cc)

    def through():
        for p in range(2):
            first = (d_right if p else d_left) * n_i + p * half
            sel = onehot(iota((half, n_j), 1) == iota((half, n_j), 0) + first)
            mko[p * half:(p + 1) * half, :] = dot_nt(sel, mkl[lanes_of(x_l if p else x_r), :].astype(F32).astype(BF16))

        def norm_via(r, carry):
            act = tbuf[r // half, r % half].astype(F32)
            mean = jnp.sum(act, axis=0, keepdims=True) * (1.0 / n_ch)
            cen = act - mean
            var = jnp.sum(cen * cen, axis=0, keepdims=True) * (1.0 / n_ch)
            nrm = cen * lax.rsqrt(var + 1e-5)
            val = (nrm * gb[0] + gb[1]).astype(BF16) * mko[pl.ds(r, 1), :].astype(BF16)
            xT[pl.ds(pl.multiple_of(r * n_ch, n_ch), n_ch), 0:s_chip] = val
            return carry

        lax.fori_loop(0, n_i, norm_via, 0, unroll=4)
        mko16 = mko[...].astype(BF16)
        for p in range(2):
            acc = dot(wbig[...], xT[p * kb:(p + 1) * kb, 0:s_chip]) + dot(bbb[p], mko16)
            bT[2, p, :, lanes_of(x_l if p else x_r)] = acc.astype(BF16)

    def step(t, carry):
        @pl.when(t == 1)
        def _():
            b_wait(1, 0)
            b_wait(1, 1)

        @pl.when(t == 2)
        def _():
            m_or.wait_recv()
            m_ol.wait_recv()
            through()
            for k in range(n_f):
                b_cut(0, k).wait_recv()
            b_fr.start()
            b_rel(2, 0).start()
            for k in range(n_f):
                b_cut(1, k).wait_recv()
            b_fl.start()
            b_rel(2, 1).start()
            for p in range(n_p):
                m_dir(0, p).start()
                m_dir(1, p).start()
                if p == 1:
                    m_fr.start()
                    m_fl.start()

        @pl.when(t == 3)
        def _():
            in_mask.wait()
            in_z.wait()
            pair_counts()
            b_wait(3, 0)
            b_wait(3, 1)

        @pl.when(t == 4)
        def _():
            b_wait(4, 0)
            b_rel(4, 0).start()
            b_wait(4, 1)
            b_rel(4, 1).start()

        @pl.when(t == 5)
        def _():
            b_wait(5, 0)
            b_wait(5, 1)

        @pl.when(t == 6)
        def _():
            b_wait(6, 0)
            b_rel(6, 0).start()
            b_wait(6, 1)
            b_rel(6, 1).start()

        @pl.when(t == 7)
        def _():
            b_wait(7, 0)
            b_wait(7, 1)

        @pl.when(t < 8)
        def _():
            compute(t)
            for f in range(2):
                y1(t, f).start()

        @pl.when(jnp.logical_and(t >= LAG1, t < 8 + LAG1))
        def _():
            v = t - LAG1
            for f in range(2):
                y1(v, f).wait_recv()

                def add(i, carry):
                    tot = rp[v, f, i].astype(F32) + rq[v, f, i].astype(F32)
                    sp[v, f, i] = tot.astype(BF16)
                    return carry

                lax.fori_loop(0, half, add, 0, unroll=4)
                y2(v, f).start()

        @pl.when(t == 8)
        def _():
            m_self.wait()
            m_land(0)
            m_land(1)
            for k in range(2):
                m_fr.wait_recv() if k == 0 else m_fl.wait_recv()
                m_p3[k].start()
            m_p0.wait_recv()
            for k in range(2):
                m_p3[k].wait_recv()
            m_part(0)
            m_part(1)

        @pl.when(t >= LAG2)
        def _():
            finish(t - LAG2)

        @pl.when(t == 9)
        def _():
            m_land(2)
            m_land(3)
            m_part(2)
            m_part(3)

        return carry

    lax.fori_loop(0, 8 + LAG2, step, 0)

    for cp in (*(b_cut(p, k) for p in range(2) for k in range(n_f)), b_r1, b_l0, b_fr, b_fl, m_or, m_ol, m_fr, m_fl, m_p0, *m_p3):
        cp.wait_send()
    for k in range(2):
        for p in range(n_p):
            m_dir(k, p).wait_send()
            m_rel(k, p).wait_send()
    for u in (0, 2, 4, 6):
        for p in range(2):
            b_rel(u, p).wait_send()

    def drain(t, carry):
        for f in range(2):
            y1(t, f).wait_send()
            y2(t, f).wait_send()
        return carry

    lax.fori_loop(0, 8, drain, 0)


def solution(mesh):
    n_y, n_d = mesh.shape["seq"], mesh.shape["dap"]
    rep = P()
    in_specs = (P(("data", "seq"), "dap", None), P("data", None), P(("data", "dap"), None, None)) + (rep,) * 8
    out_specs = (P(("data", "dap"), None, None), P(("data", "seq", "dap"), None, None))

    def local_fn(m, mask, z, gamma, beta, w_l, b_l, w_r, b_r, w_o, b_o):
        s_loc, n_i, n_ch = m.shape
        s_all, n_j = mask.shape
        n_e = w_o.shape[1]
        c_hid = w_l.shape[1]
        half = n_i // 2
        hrows = half * c_hid
        s_dev = s_loc // n_d
        vecs = [v.reshape(1, -1) for v in (gamma, beta, b_l, b_r, b_o)]
        smalls = (*vecs, w_l.T, w_r.T, w_o)
        any_spec = pl.BlockSpec(memory_space=pl.ANY)
        vm = pl.BlockSpec(memory_space=pltpu.VMEM)
        dma = pltpu.SemaphoreType.DMA
        ysh = (8, 2, half, n_i, n_e)
        mr_shape = (n_d, n_i, n_ch, s_loc * 2 // n_d)
        held = pl.pallas_call(
            functools.partial(kernel, (n_y, n_d)),
            out_shape=(pltpu.VMEM(z.shape, F32), pltpu.VMEM((s_dev, n_ch, n_j), BF16), pltpu.VMEM(mr_shape, BF16)),
            in_specs=[any_spec] * 11,
            out_specs=(vm, vm, vm),
            scratch_shapes=[pltpu.VMEM(v.shape, BF16) for v in smalls] + [
                pltpu.VMEM((n_i, n_ch, s_loc), BF16),
                pltpu.VMEM((s_all, n_j), jnp.int32),
                pltpu.VMEM((s_loc, n_j), jnp.int32),
                pltpu.VMEM((n_i * n_ch, s_loc), BF16),
                pltpu.VMEM((hrows, half * n_ch), BF16),
                pltpu.VMEM((2, hrows, n_i), BF16),
                pltpu.VMEM((n_i, s_loc), F32),
                pltpu.VMEM((4, s_loc, 256), BF16),
                pltpu.VMEM((8, 2, hrows, s_loc), BF16),
                pltpu.VMEM((c_hid * 128, 4 * n_e), BF16),
                pltpu.VMEM((16, half, c_hid * 128), BF16),
                pltpu.VMEM(ysh, BF16),
                pltpu.VMEM(ysh, BF16),
                pltpu.VMEM(ysh, BF16),
                pltpu.VMEM(ysh, BF16),
                pltpu.VMEM((n_j, 128), F32),
                pltpu.VMEM((2, half, n_ch, s_loc * 2 // n_d), BF16),
                pltpu.VMEM((2, n_ch, s_loc * 2 // n_d), F32),
                pltpu.VMEM((n_i, s_loc * 2 // n_d), F32),
                dma((5,)), dma((8,)), dma((4,)), dma((2,)), dma((8, 2)), dma((8, 2)), dma((2, 4)), dma((2, 4)),
                dma((2, 4)), dma((2,)), dma((2,)), dma((3, 4)), dma((2, 4)), dma((2,)), dma((2,)), dma((3, 4)),
                dma((8, 2)), dma((8, 2)), dma((8, 2)), dma((8, 2)),
            ],
            compiler_params=pltpu.CompilerParams(collective_id=0, has_side_effects=True, vmem_limit_bytes=52 * 2**20),
            name="opm",
        )(jnp.transpose(m, (1, 2, 0)), mask, z, *smalls)
        z_out, m_out = pl.pallas_call(
            put_out,
            out_shape=(jax.ShapeDtypeStruct(z.shape, F32), jax.ShapeDtypeStruct((s_dev, n_ch, n_j), BF16)),
            in_specs=[vm] * 3,
            out_specs=(any_spec, any_spec),
            scratch_shapes=[pltpu.VMEM((s_dev, n_ch // 4, n_j), BF16), dma((6,))],
            compiler_params=pltpu.CompilerParams(vmem_limit_bytes=10 * 2**20),
            name="out",
        )(*held)
        return z_out, jnp.transpose(m_out, (0, 2, 1))

    return jax.shard_map(local_fn, mesh=mesh, in_specs=in_specs, out_specs=out_specs, check_vma=False)
```

```python
import functools
import jax
import jax.numpy as jnp
from jax import lax
from jax.experimental import pallas as pl
from jax.experimental.pallas import tpu as pltpu
from jax.sharding import PartitionSpec as P

F32 = jnp.float32
BF16 = jnp.bfloat16
LAG1 = 1
LAG2 = 3


def iota(shape, dim):
    return lax.broadcasted_iota(jnp.int32, shape, dim)


def onehot(cond):
    return jnp.where(cond, 1.0, 0.0).astype(BF16)


def dot(a, b):
    return jnp.dot(a, b, preferred_element_type=F32)


def dot_nt(a, b):
    return lax.dot_general(a, b, (((1,), (1,)), ((), ())), preferred_element_type=F32)


def dot_tn(a, b):
    return lax.dot_general(a, b, (((0,), (0,)), ((), ())), preferred_element_type=F32)


def regroup(mr, k, chs, cc):
    _, n_i, _, s_chip = mr.shape
    per = 128 // n_i
    blk = mr[per * k:per * (k + 1), :, chs, :].astype(F32)
    blk = jnp.transpose(blk.reshape(128, blk.shape[2], s_chip), (1, 0, 2))
    blk = jnp.transpose(blk, (0, 2, 1))
    mine = jnp.where(cc == 0, blk[:, 0:s_chip // 2, :], blk[:, s_chip // 2:, :])
    return jnp.transpose(mine, (1, 0, 2)).astype(BF16)


def put_out(z_ref, o_ref, mr, zo_hbm, mo_hbm, last, sem):
    cc = lax.axis_index("dap") % 2
    n_z = z_ref.shape[0] // 8
    n_ch = o_ref.shape[1]
    ch_p = last.shape[1]
    outs = [pltpu.make_async_copy(z_ref.at[k * n_z:(k + 1) * n_z], zo_hbm.at[k * n_z:(k + 1) * n_z], sem.at[k]) for k in range(8)]
    outs.append(pltpu.make_async_copy(o_ref.at[:, 0:n_ch - ch_p], mo_hbm.at[:, 0:n_ch - ch_p], sem.at[8]))
    for o in outs:
        o.start()
    for k in range(last.shape[2] // 128):
        last[:, :, k * 128:(k + 1) * 128] = regroup(mr, k, pl.ds(n_ch - ch_p, ch_p), cc)
    tail = pltpu.make_async_copy(last, mo_hbm.at[:, n_ch - ch_p:], sem.at[9])
    tail.start()
    for o in outs + [tail]:
        o.wait()


def kernel(dims, m_hbm, mask_hbm, z_hbm, *refs):
    smalls_hbm, refs = refs[:8], refs[8:]
    (zv, ov, mr), refs = refs[:3], refs[3:]
    smalls, refs = refs[:8], refs[8:]
    gam, bet, bias_l, bias_r, bias_o, waT, wbT, wo = smalls
    (mT, mkv, mkl, xT, wbig, bbb, mkT, acat, bT, wblk, lbuf, rp, rq, sp, sq, rc, tbuf, gb, mko,
     sem_in, sem_small, bs_own, bs_fwd, bs_rel, b_recv, bs_cut, bc_recv, ms_dir, ms_opp, ms_fwd, ms_rel, m_recv, mo_recv, mf_recv, m_prel,
           y1s, y1r, y2s, y2r) = refs
    n_y, n_d = dims
    n_x = n_d // 2
    yy = lax.axis_index("seq")
    dd = lax.axis_index("dap")
    xx = dd // 2
    cc = dd % 2
    x_r = (xx + 1) % n_x
    x_l = (xx + n_x - 1) % n_x
    x_o = (xx + 2) % n_x
    right, left, mate = 2 * x_r + cc, 2 * x_l + cc, 2 * xx + 1 - cc
    par = yy % 2
    y_a = yy + 1 - 2 * par
    y_b = (yy + n_y - 1 + 2 * par) % n_y
    n_i, n_ch, s_loc = mT.shape
    s_all, n_j = mkv.shape
    c_hid = waT.shape[0]
    half = n_i // 2
    hrows = half * c_hid
    s_chip = s_loc // n_x
    s_dev = s_loc // n_d

    def to_dap(idx):
        return dict(device_id={"dap": idx}, device_id_type=pl.DeviceIdType.MESH)

    def to_seq(idx):
        return dict(device_id={"seq": idx}, device_id_type=pl.DeviceIdType.MESH)

    in_m = pltpu.make_async_copy(m_hbm, mT, sem_in.at[0])
    mine_rows = pl.ds(pl.multiple_of(yy * s_loc, s_loc), s_loc)
    in_mloc = pltpu.make_async_copy(mask_hbm.at[mine_rows], mkl, sem_in.at[4])
    in_mask = pltpu.make_async_copy(mask_hbm, mkv, sem_in.at[1])
    in_z = pltpu.make_async_copy(z_hbm, zv, sem_in.at[2])

    in_small = [pltpu.make_async_copy(a, b, sem_small.at[k]) for k, (a, b) in enumerate(zip(smalls_hbm, smalls))]

    barrier = pltpu.get_barrier_semaphore()
    for nb in (right, left, mate):
        pl.semaphore_signal(barrier, inc=1, **to_dap(nb))
    for nb in (y_a, y_b):
        pl.semaphore_signal(barrier, inc=1, **to_seq(nb))

    in_m.start()
    in_mloc.start()
    for cp in in_small:
        cp.start()

    def remote(src, dst, ssem, rsem, to):
        return pltpu.make_async_remote_copy(src_ref=src, dst_ref=dst, send_sem=ssem, recv_sem=rsem, **to)

    def lanes_of(xc):
        return pl.ds(pl.multiple_of(xc * s_chip, s_chip), s_chip)

    def b_to(src_u, src_p, dst_u, dst_p, ssem, nb):
        return remote(bT.at[src_u, src_p], bT.at[dst_u, dst_p], ssem, b_recv.at[dst_u, dst_p], to_dap(nb))

    n_f = n_x - 1

    def b_cut(p, k):
        cols = lanes_of((x_o + 1 + k) % n_x)
        src, dst = bT.at[0, p, :, cols], bT.at[2, p, :, cols]
        return remote(src, dst, bs_cut.at[p, k], bc_recv.at[p, k], to_dap(left if p else right))

    b_r1 = b_to(0, 1, 4, 0, bs_own.at[1], right)
    b_l0 = b_to(0, 0, 4, 1, bs_own.at[3], left)
    b_fr = b_to(2, 0, 6, 0, bs_fwd.at[0], right)
    b_fl = b_to(2, 1, 6, 1, bs_fwd.at[1], left)

    def b_rel(u, p):
        return b_to(u, p, u + 1, p, bs_rel.at[u, p], mate)

    def b_wait(u, p):
        b_to(u, p, u, p, bs_rel.at[u, p], mate).wait_recv()

    d_right, d_left, d_opp = 2 * x_r + cc, 2 * x_l + cc, 2 * x_o + cc
    up, lo = pl.ds(0, half), pl.ds(half, half)
    m_or = remote(m_hbm.at[up, :, lanes_of(x_o)], tbuf.at[0], ms_opp.at[0], mf_recv.at[0], to_dap(right))
    m_ol = remote(m_hbm.at[lo, :, lanes_of(x_o)], tbuf.at[1], ms_opp.at[1], mf_recv.at[1], to_dap(left))
    n_p = 4
    ch_p = n_ch // n_p

    def m_dir(k, p):
        chs = pl.ds(pl.multiple_of(p * ch_p, ch_p), ch_p)
        src = m_hbm.at[:, chs, lanes_of(x_l if k else x_r)]
        return remote(src, mr.at[dd, :, chs], ms_dir.at[k, p], m_recv.at[k, p], to_dap(left if k else right))

    def m_rel(k, p):
        chs = pl.ds(pl.multiple_of(p * ch_p, ch_p), ch_p)
        ref = mr.at[d_right if k == 0 else d_left, :, chs]
        return remote(ref, ref, ms_rel.at[k, p], m_prel.at[k, p], to_dap(mate))

    m_fr = remote(tbuf.at[0], mr.at[d_left, up], ms_fwd.at[0], mo_recv.at[0], to_dap(right))
    m_fl = remote(tbuf.at[1], mr.at[d_right, lo], ms_fwd.at[1], mo_recv.at[1], to_dap(left))
    m_p0 = remote(m_hbm.at[:, :, lanes_of(xx)], mr.at[dd], ms_rel.at[2, 0], m_prel.at[2, 0], to_dap(mate))
    m_p3 = [remote(mr.at[d_opp, rows], mr.at[d_opp, rows], ms_rel.at[2, 1 + k], m_prel.at[2, 1 + k], to_dap(mate))
            for k, rows in enumerate((up, lo))]
    m_self = pltpu.make_async_copy(m_hbm.at[:, :, lanes_of(xx)], mr.at[dd], sem_in.at[3])

    pl.semaphore_wait(barrier, 5)
    m_or.start()
    m_ol.start()
    m_p0.start()

    wblk[...] = jnp.zeros_like(wblk)

    for cp in in_small:
        cp.wait()
    def column(row, n, wide):
        eye = iota((n, n), 0) == iota((n, n), 1)
        diag = jnp.where(eye, jnp.broadcast_to(row, (n, n)), 0.0).astype(BF16)
        return dot(diag, jnp.ones((n, wide), BF16))

    lw = s_loc // 2
    gcol = column(gam[...].astype(F32), n_ch, lw)
    bcol = column(bet[...].astype(F32), n_ch, lw)
    gb[0] = gcol[:, 0:s_chip]
    gb[1] = bcol[:, 0:s_chip]
    blc = column(bias_l[...].astype(F32), c_hid, 128)
    brc = column(bias_r[...].astype(F32), c_hid, 128)
    kb = half * n_ch
    wide = dot(wbT[...], onehot((iota((n_ch, kb), 1) & (n_ch - 1)) == iota((n_ch, kb), 0)))
    keep = iota((half, kb), 0) == iota((half, kb), 1) // n_ch
    lane_i = iota((half, n_i), 1) - iota((half, n_i), 0)
    for d in range(c_hid):
        rows = slice(d * half, (d + 1) * half)
        wbig[rows, :] = jnp.where(keep, jnp.broadcast_to(wide[d:d + 1, :], (half, kb)), 0.0).astype(BF16)
        bias = jnp.broadcast_to(brc[d:d + 1, 0:n_i], (half, n_i))
        for h in range(2):
            bbb[h, rows, :] = jnp.where(lane_i == h * half, bias, 0.0).astype(BF16)

    in_mloc.wait()
    selT = onehot(iota((n_i, n_j), 1) == iota((n_i, n_j), 0) + dd * n_i)
    mkT[...] = dot_nt(selT, mkl[...].astype(F32).astype(BF16))
    in_m.wait()

    ga = 128 // c_hid
    n_e = wo.shape[1]
    pos = iota((128, c_hid * c_hid), 0)
    want = (pos & (c_hid - 1)) * c_hid + pos // c_hid
    gap = iota((128, c_hid * c_hid), 1) - want

    def place(dc, carry):
        wp = dot(onehot(gap == dc * ga), wo[...]).astype(BF16)
        for k in range(ga):
            for i4 in range(ga):
                row = pl.multiple_of((dc * ga + k) * 128 + i4 * c_hid, c_hid)
                wblk[pl.ds(row, c_hid), i4 * n_e:(i4 + 1) * n_e] = wp[k * c_hid:(k + 1) * c_hid, :]
        return carry

    def norm_row(r, carry):
        for q in range(2):
            lanes = slice(q * lw, (q + 1) * lw)
            act = mT[r, :, lanes].astype(F32)
            mean = jnp.sum(act, axis=0, keepdims=True) * (1.0 / n_ch)
            cen = act - mean
            var = jnp.sum(cen * cen, axis=0, keepdims=True) * (1.0 / n_ch)
            nrm = cen * lax.rsqrt(var + 1e-5)
            val = (nrm * gcol + bcol).astype(BF16) * mkT[pl.ds(r, 1), lanes].astype(BF16)
            xT[pl.ds(pl.multiple_of(r * n_ch, n_ch), n_ch), lanes] = val
        return carry

    mk16 = mkT[...].astype(BF16)
    for h in range(2):
        lax.fori_loop(h * half, (h + 1) * half, norm_row, 0, unroll=2)
        acc = dot(wbig[...], xT[h * kb:(h + 1) * kb, :]) + dot(bbb[h], mk16)
        bT[0, h] = acc.astype(BF16)
        if h == 0:
            for k in range(n_f):
                b_cut(0, k).start()
        else:
            for k in range(n_f):
                b_cut(1, k).start()
            b_l0.start()
            b_r1.start()
        b_rel(0, h).start()
    m_self.start()
    in_mask.start()
    in_z.start()

    ka = ga * n_ch
    ra = onehot((iota((128, c_hid), 0) & (c_hid - 1)) == iota((128, c_hid), 1))
    wa_rep = dot(dot(ra, waT[...]).astype(BF16), onehot((iota((n_ch, ka), 1) & (n_ch - 1)) == iota((n_ch, ka), 0)))
    wa4 = jnp.where(iota((128, ka), 0) // c_hid == iota((128, ka), 1) // n_ch, wa_rep, 0.0).astype(BF16)
    ba_rep = dot(ra, blc.astype(BF16))[:, 0:n_i]
    lane_a = iota((128, n_i), 1) - iota((128, n_i), 0) // c_hid
    n_g = n_i // ga
    for g in range(n_g):
        bag = jnp.where(lane_a == ga * g, ba_rep, 0.0).astype(BF16)
        at = dot(wa4, xT[g * ka:(g + 1) * ka, :]) + dot(bag, mk16)
        acat[g // 2, :, (g % 2) * 128:(g % 2 + 1) * 128] = at.T.astype(BF16)

    lax.fori_loop(0, c_hid // ga, place, 0, unroll=4)

    def pair_counts():
        sel = onehot(iota((n_j, 128), 0) == iota((n_j, 128), 1) + dd * n_i)
        rc[...] = jnp.zeros_like(rc)

        def add(k, carry):
            mk = mkv[pl.ds(pl.multiple_of(k * s_loc, s_loc), s_loc), :].astype(F32).astype(BF16)
            rc[...] += dot_tn(mk, dot(mk, sel).astype(BF16))
            return carry

        lax.fori_loop(0, s_all // s_loc, add, 0, unroll=2)
        rc[...] = 1.0 / (1e-3 + rc[...])

    def compute(t):
        lhs = bT[t].reshape(2 * hrows, s_loc)
        for n in range(4):
            acc = dot(lhs, acat[n]).astype(BF16)
            for h in range(2):
                for d in range(c_hid):
                    row = (h * c_hid + d) * half
                    for gg in range(2):
                        lbuf[(2 * n + gg) * 2 + h, :, d * 128:(d + 1) * 128] = acc[row:row + half, gg * 128:(gg + 1) * 128]
        for nn in range(2):
            cols = slice(nn * 256, (nn + 1) * 256)
            res = dot(lbuf[...].reshape(n_g * n_i, c_hid * 128), wblk[:, cols]).astype(BF16)
            for g in range(n_g):
                for k in range(2):
                    i = ga * g + 2 * nn + k
                    rp[t, i // half, i % half] = res[g * n_i:(g + 1) * n_i, k * 128:(k + 1) * 128]

    def y1(t, f):
        return remote(rp.at[t, f], rq.at[t, f], y1s.at[t, f], y1r.at[t, f], to_seq(y_a if f == 0 else y_b))

    def y2(t, f):
        return remote(sp.at[t, f], sq.at[t, f], y2s.at[t, f], y2r.at[t, f], to_seq(y_b if f == 0 else y_a))

    def j_of(t, p):
        u = t // 2
        off = jnp.where(u == 0, 0, jnp.where(u == 3, 2, n_x - 1 if p == 0 else 1))
        core = jnp.where(t % 2 == 0, cc, 1 - cc)
        hh = jnp.where(u == 2, 1 - p, p)
        return pl.multiple_of((2 * ((xx + off) % n_x) + core) * n_i + hh * half, half)

    def finish(t):
        bo = bias_o[...].astype(F32)
        for f in range(2):
            y2(t, f).wait_recv()
        for p in range(2):
            j0 = j_of(t, p)
            rcp = rc[pl.ds(j0, half), :]
            for i in range(n_i):
                rows = slice(p * half, (p + 1) * half)
                tot = sp[t, i // half, i % half, rows, :].astype(F32) + sq[t, i // half, i % half, rows, :].astype(F32)
                upd = (tot + bo) * jnp.broadcast_to(rcp[:, i:i + 1], (half, n_e))
                zv[i, pl.ds(j0, half), :] += upd

    per = 128 // n_i

    def m_land(p):
        for k in range(2):
            m_dir(k, p).wait_recv()
            m_rel(1 - k, p).start()

    def m_part(p):
        for k in range(2):
            m_rel(k, p).wait_recv()
        if p < n_p - 1:
            chs = pl.ds(p * ch_p, ch_p)
            for k in range(n_d // per):
                ov[:, chs, k * 128:(k + 1) * 128] = regroup(mr, k, chs, cc)

    def through():
        for p in range(2):
            first = (d_right if p else d_left) * n_i + p * half
            sel = onehot(iota((half, n_j), 1) == iota((half, n_j), 0) + first)
            mko[p * half:(p + 1) * half, :] = dot_nt(sel, mkl[lanes_of(x_l if p else x_r), :].astype(F32).astype(BF16))

        def norm_via(r, carry):
            act = tbuf[r // half, r % half].astype(F32)
            mean = jnp.sum(act, axis=0, keepdims=True) * (1.0 / n_ch)
            cen = act - mean
            var = jnp.sum(cen * cen, axis=0, keepdims=True) * (1.0 / n_ch)
            nrm = cen * lax.rsqrt(var + 1e-5)
            val = (nrm * gb[0] + gb[1]).astype(BF16) * mko[pl.ds(r, 1), :].astype(BF16)
            xT[pl.ds(pl.multiple_of(r * n_ch, n_ch), n_ch), 0:s_chip] = val
            return carry

        lax.fori_loop(0, n_i, norm_via, 0, unroll=4)
        mko16 = mko[...].astype(BF16)
        for p in range(2):
            acc = dot(wbig[...], xT[p * kb:(p + 1) * kb, 0:s_chip]) + dot(bbb[p], mko16)
            bT[2, p, :, lanes_of(x_l if p else x_r)] = acc.astype(BF16)

    def step(t, carry):
        @pl.when(t == 1)
        def _():
            b_wait(1, 0)
            b_wait(1, 1)

        @pl.when(t == 2)
        def _():
            m_or.wait_recv()
            m_ol.wait_recv()
            through()
            for k in range(n_f):
                b_cut(0, k).wait_recv()
            b_fr.start()
            b_rel(2, 0).start()
            for k in range(n_f):
                b_cut(1, k).wait_recv()
            b_fl.start()
            b_rel(2, 1).start()
            for p in range(n_p):
                m_dir(0, p).start()
                m_dir(1, p).start()
                if p == 1:
                    m_fr.start()
                    m_fl.start()

        @pl.when(t == 3)
        def _():
            b_wait(3, 0)
            b_wait(3, 1)

        @pl.when(t == 4)
        def _():
            in_mask.wait()
            in_z.wait()
            pair_counts()
            b_wait(4, 0)
            b_rel(4, 0).start()
            b_wait(4, 1)
            b_rel(4, 1).start()

        @pl.when(t == 5)
        def _():
            b_wait(5, 0)
            b_wait(5, 1)

        @pl.when(t == 6)
        def _():
            b_wait(6, 0)
            b_rel(6, 0).start()
            b_wait(6, 1)
            b_rel(6, 1).start()

        @pl.when(t == 7)
        def _():
            b_wait(7, 0)
            b_wait(7, 1)

        @pl.when(t < 8)
        def _():
            compute(t)
            for f in range(2):
                y1(t, f).start()

        @pl.when(jnp.logical_and(t >= LAG1, t < 8 + LAG1))
        def _():
            v = t - LAG1
            for f in range(2):
                y1(v, f).wait_recv()

                def add(i, carry):
                    tot = rp[v, f, i].astype(F32) + rq[v, f, i].astype(F32)
                    sp[v, f, i] = tot.astype(BF16)
                    return carry

                lax.fori_loop(0, half, add, 0, unroll=4)
                y2(v, f).start()

        @pl.when(t == 8)
        def _():
            m_self.wait()
            m_land(0)
            m_land(1)
            for k in range(2):
                m_fr.wait_recv() if k == 0 else m_fl.wait_recv()
                m_p3[k].start()
            m_p0.wait_recv()
            for k in range(2):
                m_p3[k].wait_recv()
            m_part(0)
            m_part(1)

        @pl.when(t == 4)
        def _():
            finish(0)

        @pl.when(t >= 4)
        def _():
            finish(t - LAG2)

        @pl.when(t == 9)
        def _():
            m_land(2)
            m_land(3)
            m_part(2)
            m_part(3)

        return carry

    lax.fori_loop(0, 8 + LAG2, step, 0)

    for cp in (*(b_cut(p, k) for p in range(2) for k in range(n_f)), b_r1, b_l0, b_fr, b_fl, m_or, m_ol, m_fr, m_fl, m_p0, *m_p3):
        cp.wait_send()
    for k in range(2):
        for p in range(n_p):
            m_dir(k, p).wait_send()
            m_rel(k, p).wait_send()
    for u in (0, 2, 4, 6):
        for p in range(2):
            b_rel(u, p).wait_send()

    def drain(t, carry):
        for f in range(2):
            y1(t, f).wait_send()
            y2(t, f).wait_send()
        return carry

    lax.fori_loop(0, 8, drain, 0)


def solution(mesh):
    n_y, n_d = mesh.shape["seq"], mesh.shape["dap"]
    rep = P()
    in_specs = (P(("data", "seq"), "dap", None), P("data", None), P(("data", "dap"), None, None)) + (rep,) * 8
    out_specs = (P(("data", "dap"), None, None), P(("data", "seq", "dap"), None, None))

    def local_fn(m, mask, z, gamma, beta, w_l, b_l, w_r, b_r, w_o, b_o):
        s_loc, n_i, n_ch = m.shape
        s_all, n_j = mask.shape
        n_e = w_o.shape[1]
        c_hid = w_l.shape[1]
        half = n_i // 2
        hrows = half * c_hid
        s_dev = s_loc // n_d
        vecs = [v.reshape(1, -1) for v in (gamma, beta, b_l, b_r, b_o)]
        smalls = (*vecs, w_l.T, w_r.T, w_o)
        any_spec = pl.BlockSpec(memory_space=pl.ANY)
        vm = pl.BlockSpec(memory_space=pltpu.VMEM)
        dma = pltpu.SemaphoreType.DMA
        ysh = (8, 2, half, n_i, n_e)
        mr_shape = (n_d, n_i, n_ch, s_loc * 2 // n_d)
        held = pl.pallas_call(
            functools.partial(kernel, (n_y, n_d)),
            out_shape=(pltpu.VMEM(z.shape, F32), pltpu.VMEM((s_dev, n_ch, n_j), BF16), pltpu.VMEM(mr_shape, BF16)),
            in_specs=[any_spec] * 11,
            out_specs=(vm, vm, vm),
            scratch_shapes=[pltpu.VMEM(v.shape, BF16) for v in smalls] + [
                pltpu.VMEM((n_i, n_ch, s_loc), BF16),
                pltpu.VMEM((s_all, n_j), jnp.int32),
                pltpu.VMEM((s_loc, n_j), jnp.int32),
                pltpu.VMEM((n_i * n_ch, s_loc), BF16),
                pltpu.VMEM((hrows, half * n_ch), BF16),
                pltpu.VMEM((2, hrows, n_i), BF16),
                pltpu.VMEM((n_i, s_loc), F32),
                pltpu.VMEM((4, s_loc, 256), BF16),
                pltpu.VMEM((8, 2, hrows, s_loc), BF16),
                pltpu.VMEM((c_hid * 128, 4 * n_e), BF16),
                pltpu.VMEM((16, half, c_hid * 128), BF16),
                pltpu.VMEM(ysh, BF16),
                pltpu.VMEM(ysh, BF16),
                pltpu.VMEM(ysh, BF16),
                pltpu.VMEM(ysh, BF16),
                pltpu.VMEM((n_j, 128), F32),
                pltpu.VMEM((2, half, n_ch, s_loc * 2 // n_d), BF16),
                pltpu.VMEM((2, n_ch, s_loc * 2 // n_d), F32),
                pltpu.VMEM((n_i, s_loc * 2 // n_d), F32),
                dma((5,)), dma((8,)), dma((4,)), dma((2,)), dma((8, 2)), dma((8, 2)), dma((2, 4)), dma((2, 4)),
                dma((2, 4)), dma((2,)), dma((2,)), dma((3, 4)), dma((2, 4)), dma((2,)), dma((2,)), dma((3, 4)),
                dma((8, 2)), dma((8, 2)), dma((8, 2)), dma((8, 2)),
            ],
            compiler_params=pltpu.CompilerParams(collective_id=0, has_side_effects=True, vmem_limit_bytes=52 * 2**20),
            name="opm",
        )(jnp.transpose(m, (1, 2, 0)), mask, z, *smalls)
        z_out, m_out = pl.pallas_call(
            put_out,
            out_shape=(jax.ShapeDtypeStruct(z.shape, F32), jax.ShapeDtypeStruct((s_dev, n_ch, n_j), BF16)),
            in_specs=[vm] * 3,
            out_specs=(any_spec, any_spec),
            scratch_shapes=[pltpu.VMEM((s_dev, n_ch // 4, n_j), BF16), dma((10,))],
            compiler_params=pltpu.CompilerParams(vmem_limit_bytes=10 * 2**20),
            name="out",
        )(*held)
        return z_out, jnp.transpose(m_out, (0, 2, 1))

    return jax.shard_map(local_fn, mesh=mesh, in_specs=in_specs, out_specs=out_specs, check_vma=False)
```
